128 devices in a mesh: data: 1, outer: 16 (over z, y), expert: 8 (over x, core).
Axes of the slice: x: 4, y: 4, z: 4, core: 2. Of those that a mesh axis runs over, the one named last changes fastest.
Arguments:
- x: bfloat16 [32768, 2048], P(('data', 'outer', 'expert'))
- wr: bfloat16 [2048, 128], replicated
- idx: int32 [32768, 8], P(('data', 'outer', 'expert'))
- w1: bfloat16 [128, 2048, 768], P(('outer', 'expert'))
- w3: bfloat16 [128, 2048, 768], P(('outer', 'expert'))
- w2: bfloat16 [128, 768, 2048], P(('outer', 'expert'))
Outputs:
- output: bfloat16 [32768, 2048], P(('data', 'outer', 'expert'))
All inputs are finite; a program needn't handle non-finite values.
Results may differ from the reference program's by a relative error of at most 0.00816633.
Values are sent between devices in bfloat16 or wider.
A program may use at most 1 GiB of HBM per device.

```python
import jax
import jax.numpy as jnp
from jax import lax

OUTER = 16
EXPERT = 8
T = 256
D = 2048
FF = 768
E = 128
TOP = 8

N_DEV = OUTER * EXPERT
CAP = 2 * T * TOP // E


def _w(key, shape, scale):
    ks = jax.random.split(key, shape[0])
    return lax.map(lambda kk: (scale * jax.random.normal(kk, shape[1:], jnp.float32)).astype(jnp.bfloat16), ks)


def setup_inputs(seed: int = 0, part: int = 0) -> dict:
    key = jax.random.key(seed)
    kr, k1, k3, k2 = jax.random.split(key, 4)
    kp = jax.random.fold_in(key, part)
    kx, _, _ = jax.random.split(kp, 3)
    kb1, kb2, kb3 = jax.random.split(jax.random.fold_in(kp, 7), 3)
    x = jax.random.normal(kx, (N_DEV * T, D), jnp.float32).astype(jnp.bfloat16)
    wr = (1.5 * D ** -0.5 * jax.random.normal(kr, (D, E), jnp.float32)).astype(jnp.bfloat16)
    w1 = _w(k1, (E, D, FF), D ** -0.5)
    w3 = _w(k3, (E, D, FF), D ** -0.5)
    w2 = _w(k2, (E, FF, D), FF ** -0.5)
    nc = N_DEV * T // E
    rot = jax.random.randint(kb1, (N_DEV,), 0, E, jnp.int32)
    base = jnp.arange(E, dtype=jnp.int32) // 2
    p = jax.vmap(lambda kk: jax.random.permutation(kk, base))(jax.random.split(kb2, nc))
    p = p + jnp.repeat(rot, T // E)[:, None]
    w = min(2 * TOP, E)
    off = jax.vmap(lambda kk: jax.random.permutation(kk, w)[:TOP])(jax.random.split(kb3, nc))
    idx = ((p[:, :, None] + off[:, None, :]) % E).reshape(N_DEV * T, TOP).astype(jnp.int32)
    return {'x': x, 'wr': wr, 'idx': idx, 'w1': w1, 'w3': w3, 'w2': w2}


def _ranks(e, num):
    order = jnp.argsort(e, stable=True)
    se = e[order]
    first = jnp.searchsorted(se, jnp.arange(num, dtype=jnp.int32), side='left').astype(jnp.int32)
    r = jnp.arange(e.shape[0], dtype=jnp.int32) - first[se]
    return jnp.zeros_like(e).at[order].set(r)


def reference(x, wr, idx, w1, w3, w2):
    logits = jnp.dot(x, wr, preferred_element_type=jnp.float32)
    g = jax.nn.softmax(jnp.take_along_axis(logits, idx, axis=1), axis=-1)
    eb = idx.reshape(N_DEV, T * TOP)
    r = jax.vmap(lambda v: _ranks(v, E))(eb).reshape(-1)
    e = eb.reshape(-1)
    src = jnp.arange(N_DEV * T * TOP, dtype=jnp.int32) // (T * TOP)
    tok = jnp.arange(N_DEV * T * TOP, dtype=jnp.int32) // TOP
    pos = jnp.where(r < CAP, e * (N_DEV * CAP) + src * CAP + r, E * N_DEV * CAP)
    tab = jnp.full((E * N_DEV * CAP,), N_DEV * T, jnp.int32).at[pos].set(tok, mode='drop').reshape(E, N_DEV * CAP)
    gt = jnp.zeros((E * N_DEV * CAP,), jnp.float32).at[pos].set(g.reshape(-1), mode='drop').reshape(E, N_DEV * CAP)

    def step(y, inp):
        t, gw, a1, a3, a2 = inp
        xe = jnp.take(x, t, axis=0, mode='fill', fill_value=0)
        a = jnp.dot(xe, a1, preferred_element_type=jnp.float32)
        b = jnp.dot(xe, a3, preferred_element_type=jnp.float32)
        h = (jax.nn.silu(a) * b).astype(jnp.bfloat16)
        o = jnp.dot(h, a2, preferred_element_type=jnp.float32).astype(jnp.bfloat16)
        return y.at[t].add(gw[:, None] * o.astype(jnp.float32), mode='drop'), None

    y, _ = lax.scan(step, jnp.zeros((N_DEV * T, D), jnp.float32), (tab, gt, w1, w3, w2))
    return y.astype(jnp.bfloat16)
```

```python
import jax
import jax.numpy as jnp
from jax import lax
from jax.sharding import PartitionSpec as P


def _gate(x, wr, idx):
    logits = jnp.dot(x, wr, preferred_element_type=jnp.float32)
    oh = idx[:, :, None] == jnp.arange(wr.shape[1], dtype=idx.dtype)
    return jax.nn.softmax(jnp.sum(jnp.where(oh, logits[:, None, :], 0.0), axis=-1), axis=-1)


def _plan(idx, g, base, ne, cap):
    t = idx.shape[-2]
    oh = idx[..., None] == base + jnp.arange(ne, dtype=idx.dtype)
    m = jnp.sum(oh, axis=-2, dtype=jnp.int32).astype(jnp.float32)
    pos = jnp.arange(t, dtype=jnp.int32)
    tri = (pos[None, :] < pos[:, None]).astype(jnp.bfloat16)
    cnt = jnp.einsum('uv,...ve->...ue', tri, m.astype(jnp.bfloat16), preferred_element_type=jnp.float32)
    c = jnp.arange(cap, dtype=jnp.float32)
    hit = (c >= cnt[..., None]) & (c < (cnt + m)[..., None])
    ge = jnp.sum(jnp.where(oh, g[..., None], 0.0), axis=-2)
    w = jnp.where(hit, ge[..., None], 0.0)
    return hit.astype(jnp.bfloat16), w


def _split(w):
    hi = w.astype(jnp.bfloat16)
    r = w - hi.astype(jnp.float32)
    mid = r.astype(jnp.bfloat16)
    lo = (r - mid.astype(jnp.float32)).astype(jnp.bfloat16)
    return jnp.stack([hi, mid, lo])


def solution(mesh):
    O = mesh.shape['outer']
    X = mesh.shape['expert']
    n = O * X
    tok = P(('data', 'outer', 'expert'), None)
    wsp = P(('outer', 'expert'), None, None)

    def local(x, wr, idx, w1, w3, w2):
        T, dm = x.shape
        k = idx.shape[1]
        E = wr.shape[1]
        el = w1.shape[0]
        C = 2 * T * k // E
        g = _gate(x, wr, idx)
        hit, w = _plan(idx, g, 0, E, C)
        ws = _split(w).reshape(3 * T, E * C)
        buf = jnp.einsum('tec,td->ecd', hit, x, preferred_element_type=jnp.float32).astype(x.dtype)
        buf = buf.reshape(n, el * C, dm)
        buf = lax.all_to_all(buf, ('outer', 'expert'), 0, 0, tiled=True)
        xin = buf.reshape(n, el, C, dm).transpose(1, 0, 2, 3).reshape(el, n * C, dm)
        a = jnp.einsum('ecd,edf->ecf', xin, w1, preferred_element_type=jnp.float32)
        b = jnp.einsum('ecd,edf->ecf', xin, w3, preferred_element_type=jnp.float32)
        h = (jax.nn.silu(a) * b).astype(jnp.bfloat16)
        o = jnp.einsum('ecf,efd->ecd', h, w2, preferred_element_type=jnp.float32).astype(jnp.bfloat16)
        o = o.reshape(el, n, C, dm).transpose(1, 0, 2, 3).reshape(n, el * C, dm)
        o = lax.all_to_all(o, ('outer', 'expert'), 0, 0, tiled=True)
        y = jnp.dot(ws, o.reshape(E * C, dm), preferred_element_type=jnp.float32)
        return jnp.sum(y.reshape(3, T, dm), axis=0).astype(jnp.bfloat16)

    return jax.shard_map(local, mesh=mesh, in_specs=(tok, P(None, None), tok, wsp, wsp, wsp), out_specs=tok, check_vma=False)
```

```python
import functools

import jax
import jax.numpy as jnp
from jax import lax
from jax.experimental import pallas as pl
from jax.experimental.pallas import tpu as pltpu
from jax.sharding import PartitionSpec as P

MESH = pl.DeviceIdType.MESH
F32 = jnp.float32
BF16 = jnp.bfloat16


def _cols(d):
    t = d // 128
    w = [(t // 3) * 128, (t // 3) * 128, (t - 2 * (t // 3)) * 128]
    return [(0, w[0]), (w[0], w[1]), (w[0] + w[1], w[2])]


def _where(n):
    o, e = lax.axis_index('outer'), lax.axis_index('expert')
    return o // n, o % n, e // 2, e % 2


def _dev(n, z, y, x, c):
    return (0, z * n + y, x * 2 + c)


def _along(n, p, me, a):
    z, y, x, c = me
    return _dev(n, *((a, y, x, c), (z, a, x, c), (z, y, a, c))[p])


def _copy(src, dst, send, recv, dev):
    return pltpu.make_async_remote_copy(src_ref=src, dst_ref=dst, send_sem=send, recv_sem=recv, device_id=dev, device_id_type=MESH)


def _wait(ref, sem):
    pltpu.make_async_copy(ref, ref, sem).wait()


def _dispatch(n, cols, x_ref, meta_ref, xin, meta_out, ag0, ag1, ag2, mb, sb0, sb1, sb2, own, asend, msend, arecv, mrecv, send, recv):
    me = _where(n)
    z, y, x, c = me
    ag, sb = (ag0, ag1, ag2), (sb0, sb1, sb2)
    T = x_ref.shape[0]
    C = sb0.shape[2]
    L = 2 * n * C
    axis = (z, y, x)
    which = (0, 0, 1)
    ring = [1, n - 1] + list(range(2, n - 1)) if n > 2 else [1]
    for p in range(3):
        lo, w = cols[p]
        for k in ring:
            to = _along(n, p, me, (axis[p] + k) % n)
            _copy(meta_ref.at[which[p]], mb.at[p, axis[p]], msend.at[p, k], mrecv.at[p, k], to).start()
            _copy(x_ref.at[:, pl.ds(lo, w)], ag[p].at[axis[p]], asend.at[p, k], arecv.at[p, k], to).start()
        pltpu.make_async_copy(meta_ref.at[which[p]], mb.at[p, axis[p]], msend.at[p, 0]).start()
        pltpu.make_async_copy(x_ref.at[:, pl.ds(lo, w)], ag[p].at[axis[p]], asend.at[p, 0]).start()

    for p in range(3):
        lo, w = cols[p]
        _wait(mb.at[p, 0], msend.at[p, 0])
        _wait(ag[p].at[0], asend.at[p, 0])
        for k in ring:
            _wait(mb.at[p, 0], mrecv.at[p, k])
            _wait(ag[p].at[0], arecv.at[p, k])

        @pl.loop(0, n)
        def _(i):
            b = ((y, z, z)[p] + i) % n
            row = (z * n + b, b * n + y, b * n + x)[p]
            for a in range(n):
                tab = mb[p, a, 0, pl.ds(row, 1), :]
                hot = lax.broadcasted_iota(jnp.int32, (T, L), 0).astype(F32) == tab
                hot = jnp.where(hot, 1.0, 0.0).astype(BF16)
                r = lax.dot_general(hot, ag[p][a], (((0,), (0,)), ((), ())), preferred_element_type=F32)
                sb[p][a, pl.ds(b * 2 * n, 2 * n)] = r.astype(BF16).reshape(2 * n, C, w)
            for jj in range(2 * n):
                d = ((x, x, y)[p] + jj // 2) % n
                cc = (c + jj) % 2
                to = _dev(n, *((z, b, d, cc), (b, y, d, cc), (b, d, x, cc))[p])
                src = sb[p].at[:, b * 2 * n + d * 2 + cc]
                dst = (xin.at[:, y, x, c, :, pl.ds(lo, w)], xin.at[z, :, x, c, :, pl.ds(lo, w)], xin.at[z, y, :, c, :, pl.ds(lo, w)])[p]
                far = _copy(src, dst, send.at[p], recv.at[p], to)
                if jj:
                    far.start()
                else:
                    @pl.when(i == 0)
                    def _():
                        pltpu.make_async_copy(src, dst, own.at[p]).start()

                    @pl.when(i > 0)
                    def _():
                        far.start()

    meta_out[...] = mb[...]
    for p in range(3):
        rest = sb[p].at[:, pl.ds(0, 2 * n * n - 1)]
        for k in ring:
            _wait(mb.at[p, 0], msend.at[p, k])
            _wait(ag[p].at[0], asend.at[p, k])
        _wait(sb[p].at[:, 0], own.at[p])
        _wait(rest, send.at[p])
        _wait(rest, recv.at[p])


def _experts(n, cols, xin, w1_ref, w3_ref, w2_ref, r0, r1, r2, w1, w3, w2, xb, hb, ob, wsem, xsem, own, send, recv):
    me = _where(n)
    z, y, x, c = me
    R = (r0, r1, r2)
    C, D = xin.shape[4:]
    G = 2 * n * C
    ff = w1.shape[1]
    half = n // 2
    steps = n * half
    loads = [pltpu.make_async_copy(s.at[0], d, wsem.at[q]) for q, (s, d) in enumerate(((w1_ref, w1), (w3_ref, w3), (w2_ref, w2)))]

    def place(s):
        jp = s % half
        return (z + s // half) % n, (y + 2 * jp) % n, (y + 2 * jp + 1) % n

    def load(s):
        zt, y0, y1 = place(s)
        return [pltpu.make_async_copy(xin.at[zt, yv], xb.at[s % 2, q], xsem.at[s % 2, q]) for q, yv in enumerate((y0, y1))]

    for q in load(0):
        q.start()
    for q in loads:
        q.start()
    mine = (y * 2 * n + x * 2 + c, z * 2 * n + x * 2 + c, z * 2 * n + y * 2 + c)

    def out(p, src, dst, to, local):
        far = _copy(src, dst, send.at[p], recv.at[p], to)
        if local is None:
            far.start()
            return

        @pl.when(local)
        def _():
            pltpu.make_async_copy(src, dst, own.at[p]).start()

        @pl.when(jnp.logical_not(local))
        def _():
            far.start()

    fs, ds = min(256, ff), min(512, D)
    cs = [pl.ds(lo, w) for lo, w in cols]

    @pl.loop(0, steps)
    def _(s):
        zt, y0, y1 = place(s)
        i, jp = s // half, s % half

        @pl.when(s + 1 < steps)
        def _():
            for q in load(s + 1):
                q.start()

        for q in load(s):
            q.wait()

        @pl.when(s == 0)
        def _():
            for q in loads:
                q.wait()

        @pl.loop(0, ff // fs)
        def _(f):
            fc = pl.ds(pl.multiple_of(f * fs, fs), fs)
            xt = xb[s % 2].reshape(2 * G, D)
            a = jnp.dot(xt, w1[:, fc], preferred_element_type=F32)
            b = jnp.dot(xt, w3[:, fc], preferred_element_type=F32)
            hb[:, fc] = (jax.nn.silu(a) * b).astype(BF16)

        @pl.loop(0, D // ds)
        def _(f):
            fc = pl.ds(pl.multiple_of(f * ds, ds), ds)
            o = jnp.dot(hb[...], w2[:, fc], preferred_element_type=F32).astype(BF16)
            ob[zt, y0, :, :, :, fc] = o[:G].reshape(n, 2, C, ds)
            ob[zt, y1, :, :, :, fc] = o[G:].reshape(n, 2, C, ds)

        for q, yv in enumerate((y0, y1)):
            for cc in range(2):
                c2 = (c + cc) % 2
                out(2, ob.at[zt, yv, :, c2, :, cs[2]], R[2].at[:, mine[2]], _dev(n, zt, yv, x, c2), (s == 0) if q + cc == 0 else None)
            for d in range(n):
                for cc in range(2):
                    x2, c2 = (x + d) % n, (c + cc) % 2
                    out(0, ob.at[zt, yv, x2, c2, :, cs[0]], R[0].at[zt, mine[0]], _dev(n, z, yv, x2, c2), (jp == 0) if q + d + cc == 0 else None)

        @pl.when(jp == half - 1)
        def _():
            for d in range(n):
                for cc in range(2):
                    x2, c2 = (x + d) % n, (c + cc) % 2
                    out(1, ob.at[zt, :, x2, c2, :, cs[1]], R[1].at[:, mine[1]], _dev(n, zt, y, x2, c2), (i == 0) if d + cc == 0 else None)

    for p in range(3):
        rest = R[p].at[:, pl.ds(0, 2 * n * n - 1)]
        _wait(R[p].at[:, 0], own.at[p])
        _wait(rest, send.at[p])
        _wait(rest, recv.at[p])


def _combine(n, cols, r0, r1, r2, meta, y_ref, b0, b1, b2, p0, p1, p2, q0, q1, q2, rsem, send, recv):
    me = _where(n)
    z, y, x, c = me
    R, B, S, Q = (r0, r1, r2), (b0, b1, b2), (p0, p1, p2), (q0, q1, q2)
    axis = (z, y, x)
    T = y_ref.shape[0]
    C = b0.shape[2]
    L = 2 * n * C
    for p in range(3):
        pltpu.make_async_copy(R[p], B[p], rsem.at[p]).start()
    for p in range(3):
        lo, w = cols[p]
        _wait(B[p], rsem.at[p])

        @pl.loop(0, n)
        def _(k):
            k = (k + 1) % n
            a = (axis[p] + k) % n

            for b in range(n):
                row = (z * n + b, b * n + y, b * n + x)[p]
                tab = meta[p, a, 0, pl.ds(row, 1), :]
                g = meta[p, a, 1, pl.ds(row, 1), :]
                hot = lax.broadcasted_iota(jnp.int32, (T, L), 0).astype(F32) == tab
                m = jnp.where(hot, g, 0.0)
                hi = m.astype(BF16)
                m = m - hi.astype(F32)
                mid = m.astype(BF16)
                low = (m - mid.astype(F32)).astype(BF16)
                v = B[p][a, pl.ds(b * 2 * n, 2 * n)].reshape(L, w)
                t = jnp.dot(hi, v, preferred_element_type=F32)
                t += jnp.dot(mid, v, preferred_element_type=F32)
                t += jnp.dot(low, v, preferred_element_type=F32)
                if b == 0:
                    S[p][k] = t
                else:
                    S[p][k] += t

            @pl.when(k > 0)
            def _():
                _copy(S[p].at[k], Q[p].at[k - 1], send.at[p, k], recv.at[p, k], _along(n, p, me, a)).start()

    for p in range(3):
        lo, w = cols[p]
        t = S[p][0]
        for k in range(1, n):
            _wait(Q[p].at[k - 1], recv.at[p, k])
            t += Q[p][k - 1]
        y_ref[:, pl.ds(lo, w)] = t.astype(BF16)
    for p in range(3):
        for k in range(1, n):
            _wait(Q[p].at[k - 1], send.at[p, k])


def _plan(x, wr, idx, n, cap):
    T = x.shape[0]
    E = wr.shape[1]
    logits = jnp.dot(x, wr, preferred_element_type=F32)
    oh = idx[:, :, None] == jnp.arange(E, dtype=idx.dtype)
    g = jax.nn.softmax(jnp.sum(jnp.where(oh, logits[:, None, :], 0.0), axis=-1), axis=-1)
    m = jnp.sum(oh, axis=1, dtype=jnp.int32).astype(F32)
    ge = jnp.sum(jnp.where(oh, g[:, :, None], 0.0), axis=1)
    pos = jnp.arange(T, dtype=jnp.int32)
    tri = (pos[None, :] < pos[:, None]).astype(BF16)
    cnt = jnp.dot(tri, m.astype(BF16), preferred_element_type=F32)
    cnt = jnp.where(m > 0, cnt, -1.0)
    hit = cnt[:, :, None] == jnp.arange(cap, dtype=F32)
    tab = jnp.sum(jnp.where(hit, pos.astype(F32)[:, None, None] + 1.0, 0.0), axis=0) - 1.0
    gw = jnp.sum(jnp.where(hit, ge[:, :, None], 0.0), axis=0)

    def both(v):
        v = v.reshape(n, n, n, 2 * cap)
        return v.reshape(n * n, 2 * n * cap), v.transpose(0, 2, 1, 3).reshape(n * n, 2 * n * cap)

    (t0, t2), (g0, g2) = both(tab), both(gw)
    return jnp.stack([jnp.stack([t0, g0]), jnp.stack([t2, g2])])


def solution(mesh):
    O, X = mesh.shape['outer'], mesh.shape['expert']
    n = X // 2
    tok = P(('data', 'outer', 'expert'), None)
    wsp = P(('outer', 'expert'), None, None)
    any_ = pl.BlockSpec(memory_space=pl.ANY)
    vmem = pl.BlockSpec(memory_space=pltpu.VMEM)
    dma = pltpu.SemaphoreType.DMA
    params = pltpu.CompilerParams(has_side_effects=True, vmem_limit_bytes=60 * 1024 * 1024)

    def local(x, wr, idx, w1, w3, w2):
        T, D = x.shape
        E = wr.shape[1]
        C = 2 * T * idx.shape[1] // E
        ff = w1.shape[2]
        cols = _cols(D)
        widths = [w for _, w in cols]
        L = 2 * n * C
        blocks = [(n, 2 * n * n, C, w) for w in widths]
        meta = _plan(x, wr, idx, n, C)
        xin, metas = pl.pallas_call(
            functools.partial(_dispatch, n, cols),
            name='dispatch',
            out_shape=[jax.ShapeDtypeStruct((n, n, n, 2, C, D), BF16), jax.ShapeDtypeStruct((3, n, 2, n * n, L), F32)],
            in_specs=[any_, any_],
            out_specs=[any_, vmem],
            scratch_shapes=[pltpu.VMEM((n, T, w), BF16) for w in widths] + [pltpu.VMEM((3, n, 2, n * n, L), F32)]
            + [pltpu.VMEM(b, BF16) for b in blocks]
            + [dma((3,)), dma((3, n)), dma((3, n)), dma((3, n)), dma((3, n)), dma((3,)), dma((3,))],
            compiler_params=params,
        )(x, meta)
        r = pl.pallas_call(
            functools.partial(_experts, n, cols),
            name='experts',
            out_shape=[jax.ShapeDtypeStruct(b, BF16) for b in blocks],
            in_specs=[any_] * 4,
            out_specs=[any_] * 3,
            scratch_shapes=[
                pltpu.VMEM((D, ff), BF16), pltpu.VMEM((D, ff), BF16), pltpu.VMEM((ff, D), BF16),
                pltpu.VMEM((2, 2, n, 2, C, D), BF16), pltpu.VMEM((2 * L, ff), BF16), pltpu.VMEM((n, n, n, 2, C, D), BF16),
                dma((3,)), dma((2, 2)), dma((3,)), dma((3,)), dma((3,)),
            ],
            compiler_params=params,
        )(xin, w1, w3, w2)
        return pl.pallas_call(
            functools.partial(_combine, n, cols),
            name='combine',
            out_shape=jax.ShapeDtypeStruct((T, D), BF16),
            in_specs=[any_] * 3 + [vmem],
            out_specs=vmem,
            scratch_shapes=[pltpu.VMEM(b, BF16) for b in blocks]
            + [pltpu.VMEM((n, T, w), F32) for w in widths] + [pltpu.VMEM((n - 1, T, w), F32) for w in widths]
            + [dma((3,)), dma((3, n)), dma((3, n))],
            compiler_params=params,
        )(*r, metas)

    return jax.shard_map(local, mesh=mesh, in_specs=(tok, P(None, None), tok, wsp, wsp, wsp), out_specs=tok, check_vma=False)
```

```python
import functools

import jax
import jax.numpy as jnp
from jax import lax
from jax.experimental import pallas as pl
from jax.experimental.pallas import tpu as pltpu
from jax.sharding import PartitionSpec as P

MESH = pl.DeviceIdType.MESH
F32 = jnp.float32
BF16 = jnp.bfloat16
N = 4


def _cols(d):
    t = d // 128
    w = [(t // 3) * 128, (t // 3) * 128, (t - 2 * (t // 3)) * 128]
    return [(0, w[0]), (w[0], w[1]), (w[0] + w[1], w[2])]


def _where():
    o, e = lax.axis_index('outer'), lax.axis_index('expert')
    return o // N, o % N, e // 2, e % 2


def _dev(z, y, x, c):
    return (0, z * N + y, x * 2 + c)


def _along(p, me, a):
    z, y, x, c = me
    return _dev(*((a, y, x, c), (z, a, x, c), (z, y, a, c))[p])


def _plane(p, me, b, d, c):
    z, y, x, _ = me
    return _dev(*((z, b, d, c), (b, y, d, c), (b, d, x, c))[p])


def _copy(src, dst, send, recv, dev):
    return pltpu.make_async_remote_copy(src_ref=src, dst_ref=dst, send_sem=send, recv_sem=recv, device_id=dev, device_id_type=MESH)


def _wait(ref, sem):
    pltpu.make_async_copy(ref, ref, sem).wait()


def _far(o):
    return int(o == 2)


RELAYED = [(b, d, cc) for b in (2, 1, 3, 0) for d in (2, 1, 3, 0) for cc in range(2) if 2 in (b, d)]
NEAR = N * N * 2 - len(RELAYED) - 1


def _forward(p, me, base, rel, rsem, final, fsend, recv):
    c = me[3]
    for b, d, cc in RELAYED:
        s = 1 - 2 * cc
        bs, ds = (base[0] + N - s * _far(b)) % N, (base[1] + N - s * _far(d)) % N
        key = (b * N + d) * 2 + cc
        _wait(rel.at[:, key], rsem.at[p, key])
        to = _plane(p, me, (bs + b) % N, (ds + d) % N, (c + cc) % 2)
        _copy(rel.at[:, key], final(p, bs, ds), fsend.at[p], recv.at[p], to).start()


def _dispatch(cols, x_ref, meta_ref, xin, meta_out, ag0, ag1, ag2, mb, sb0, sb1, sb2, rl0, rl1, rl2,
              own, lown, asend, msend, arecv, mrecv, lsend, send, fsend, rrecv, recv):
    me = _where()
    z, y, x, c = me
    ag, sb, rl = (ag0, ag1, ag2), (sb0, sb1, sb2), (rl0, rl1, rl2)
    T = x_ref.shape[0]
    C = sb0.shape[2]
    L = 2 * N * C
    h = T // 2
    axis = (z, y, x)
    base = ((y, x), (z, x), (z, y))
    which = (0, 0, 1)
    for p in range(3):
        lo, w = cols[p]
        at = axis[p]
        blk = x_ref.at[:, pl.ds(lo, w)]
        for k in range(2):
            _copy(blk, ag[p].at[at], asend.at[p, k], arecv.at[p, k], _along(p, me, (at + (1, 3)[k]) % N)).start()
        pltpu.make_async_copy(blk, ag[p].at[at], lown.at[p, 0]).start()
    for p in range(3):
        at = axis[p]
        for k in (1, 3, 2):
            _copy(meta_ref.at[which[p]], mb.at[p, at], msend.at[p, k], mrecv.at[p, k], _along(p, me, (at + k) % N)).start()
        pltpu.make_async_copy(meta_ref.at[which[p]], mb.at[p, at], lown.at[p, 1]).start()
    halves = (pl.ds(0, h), pl.ds(h, h))
    for p in range(3):
        at = axis[p]
        for k in range(2):
            _wait(ag[p].at[0], arecv.at[p, k])
            part = ag[p].at[(at + (3, 1)[k]) % N, halves[k]]
            _copy(part, part, asend.at[p, 2 + k], arecv.at[p, 2 + k], _along(p, me, (at + (1, 3)[k]) % N)).start()

    def final(p, b, d):
        cs = pl.ds(*cols[p])
        return (xin.at[:, b, d, c, :, cs], xin.at[b, :, d, c, :, cs], xin.at[b, d, :, c, :, cs])[p]

    for p in range(3):
        w = cols[p][1]
        bm, dm = base[p]
        _wait(mb.at[p, 0], lown.at[p, 1])
        _wait(ag[p].at[0], lown.at[p, 0])
        for k in (1, 3, 2):
            _wait(mb.at[p, 0], mrecv.at[p, k])
        for k in range(2):
            _wait(ag[p].at[0, halves[k]], arecv.at[p, 2 + k])

        @pl.loop(0, N)
        def _(i):
            bo = (2 + 3 * i) % N
            b = (bm + bo) % N
            row = (z * N + b, b * N + y, b * N + x)[p]

            for a in range(N):
                tab = mb[p, a, 0, pl.ds(row, 1), :]
                hot = lax.broadcasted_iota(jnp.int32, (T, L), 0).astype(F32) == tab
                hot = jnp.where(hot, 1.0, 0.0).astype(BF16)
                r = lax.dot_general(hot, ag[p][a], (((0,), (0,)), ((), ())), preferred_element_type=F32)
                sb[p][a, pl.ds(b * 2 * N, 2 * N)] = r.astype(BF16).reshape(2 * N, C, w)
            for do in (2, 1, 3, 0):
                for cc in range(2):
                    s = 1 - 2 * cc
                    d = (dm + do) % N
                    fb = (N - 1 - i) // (N - 1)
                    to = _plane(p, me, (bm + N + s * fb) % N, (dm + N + s * _far(do)) % N, c)
                    leg = _copy(sb[p].at[:, b * 2 * N + d * 2 + (c + cc) % 2], rl[p].at[:, (bo * N + do) * 2 + cc],
                                lsend.at[p], rrecv.at[p, (bo * N + do) * 2 + cc], to)
                    if _far(do):
                        leg.start()
                    else:
                        @pl.when(i == 0)
                        def _():
                            leg.start()

    for bo in (1, 3, 0):
        for do in (1, 3, 0):
            for cc in range(2):
                for p in range(3):
                    bm, dm = base[p]
                    b, d, c2 = (bm + bo) % N, (dm + do) % N, (c + cc) % 2
                    src = sb[p].at[:, b * 2 * N + d * 2 + c2]
                    if bo + do + cc == 0:
                        pltpu.make_async_copy(src, final(p, bm, dm), own.at[p]).start()
                    else:
                        _copy(src, final(p, bm, dm), send.at[p], recv.at[p], _plane(p, me, b, d, c2)).start()
    meta_out[...] = mb[...]
    for p in range(3):
        _forward(p, me, base[p], rl[p], rrecv, final, fsend, recv)
    for p in range(3):
        for k in (1, 2, 3):
            _wait(mb.at[p, 0], msend.at[p, k])
        for k in range(2):
            _wait(ag[p].at[0], asend.at[p, k])
            _wait(ag[p].at[0, halves[k]], asend.at[p, 2 + k])
        _wait(sb[p].at[:, 0], own.at[p])
        _wait(sb[p].at[:, pl.ds(0, NEAR)], send.at[p])
        _wait(sb[p].at[:, pl.ds(0, len(RELAYED))], lsend.at[p])
        _wait(sb[p].at[:, pl.ds(0, len(RELAYED))], fsend.at[p])
        _wait(sb[p].at[:, pl.ds(0, NEAR + len(RELAYED))], recv.at[p])


def _experts(cols, xin, w1_ref, w3_ref, w2_ref, r0, r1, r2, w1, w3, w2, xb, hb, ob, rl0, rl1, rl2,
             wsem, xsem, own, lsend, send, fsend, rrecv, recv):
    me = _where()
    z, y, x, c = me
    R, rl = (r0, r1, r2), (rl0, rl1, rl2)
    C, D = xin.shape[4:]
    G = 2 * N * C
    ff = w1.shape[1]
    half = N // 2
    steps = N * half
    base = ((y, x), (z, x), (z, y))
    loads = [pltpu.make_async_copy(s.at[0], d, wsem.at[q]) for q, (s, d) in enumerate(((w1_ref, w1), (w3_ref, w3), (w2_ref, w2)))]

    def place(s):
        zo = (2 + 3 * (s // half)) % N
        yo = [(2 + 2 * (s % half) + 3 * q) % N for q in range(2)]
        return (z + zo) % N, zo, [(y + o) % N for o in yo], yo

    def load(s):
        zt, _, ys, _ = place(s)
        return [pltpu.make_async_copy(xin.at[zt, yv], xb.at[s % 2, q], xsem.at[s % 2, q]) for q, yv in enumerate(ys)]

    for q in load(0):
        q.start()
    for q in loads:
        q.start()
    cs = [pl.ds(lo, w) for lo, w in cols]

    def final(p, b, d):
        return R[p].at[:, (b * N + d) * 2 + c]

    def put(p, src, bo, do, fb, fd, cc, lead, relay, self_):
        bm, dm = base[p]
        s = 1 - 2 * cc
        key = (bo * N + do) * 2 + cc
        leg = _copy(src, rl[p].at[lead, key], lsend.at[p], rrecv.at[p, key],
                    _plane(p, me, (bm + N + s * fb) % N, (dm + N + s * fd) % N, c))
        dst = R[p].at[lead, (bm * N + dm) * 2 + c]
        far = _copy(src, dst, send.at[p], recv.at[p], _plane(p, me, (bm + bo) % N, (dm + do) % N, (c + cc) % 2))
        near = pltpu.make_async_copy(src, dst, own.at[p])
        if relay is True:
            leg.start()
            return

        def direct():
            if self_ is None:
                far.start()
                return

            @pl.when(self_)
            def _():
                near.start()

            @pl.when(jnp.logical_not(self_))
            def _():
                far.start()

        if relay is None:
            direct()
            return

        @pl.when(relay)
        def _():
            leg.start()

        @pl.when(jnp.logical_not(relay))
        def _():
            direct()

    fs, ds = min(256, ff), min(512, D)
    every = slice(None)

    @pl.loop(0, steps)
    def _(s):
        zt, zo, ys, yo = place(s)
        i, jp = s // half, s % half
        fz = (N - 1 - i) // (N - 1)

        @pl.when(s + 1 < steps)
        def _():
            for q in load(s + 1):
                q.start()

        for q in load(s):
            q.wait()

        @pl.when(s == 0)
        def _():
            for q in loads:
                q.wait()

        @pl.loop(0, ff // fs)
        def _(f):
            fc = pl.ds(pl.multiple_of(f * fs, fs), fs)
            xt = xb[s % 2].reshape(2 * G, D)
            a = jnp.dot(xt, w1[:, fc], preferred_element_type=F32)
            b = jnp.dot(xt, w3[:, fc], preferred_element_type=F32)
            hb[:, fc] = (jax.nn.silu(a) * b).astype(BF16)

        @pl.loop(0, D // ds)
        def _(f):
            fc = pl.ds(pl.multiple_of(f * ds, ds), ds)
            o = jnp.dot(hb[...], w2[:, fc], preferred_element_type=F32).astype(BF16)
            ob[zt, ys[0], :, :, :, fc] = o[:G].reshape(N, 2, C, ds)
            ob[zt, ys[1], :, :, :, fc] = o[G:].reshape(N, 2, C, ds)

        for q in range(2):
            fy = 1 - jp if q == 0 else 0
            for cc in range(2):
                put(2, ob.at[zt, ys[q], :, (c + cc) % 2, :, cs[2]], zo, yo[q], fz, fy, cc, every,
                    (i == 0) if q else (fz + fy > 0), (s == 2 * half + 1) if q + cc == 0 else None)
            for do in (2, 1, 3, 0):
                for cc in range(2):
                    put(0, ob.at[zt, ys[q], (x + do) % N, (c + cc) % 2, :, cs[0]], yo[q], do, fy, _far(do), cc, zt,
                        True if _far(do) else (None if q else (jp == 0)), (jp == 1) if q + do + cc == 0 else None)

        @pl.when(jp == half - 1)
        def _():
            for do in (2, 1, 3, 0):
                for cc in range(2):
                    put(1, ob.at[zt, :, (x + do) % N, (c + cc) % 2, :, cs[1]], zo, do, fz, _far(do), cc, every,
                        True if _far(do) else (i == 0), (i == 2) if do + cc == 0 else None)

    for p in (2, 1, 0):
        _forward(p, me, base[p], rl[p], rrecv, final, fsend, recv)
    for p in range(3):
        _wait(R[p].at[:, 0], own.at[p])
        _wait(R[p].at[:, pl.ds(0, NEAR)], send.at[p])
        _wait(R[p].at[:, pl.ds(0, len(RELAYED))], lsend.at[p])
        _wait(R[p].at[:, pl.ds(0, len(RELAYED))], fsend.at[p])
        _wait(R[p].at[:, pl.ds(0, NEAR + len(RELAYED))], recv.at[p])


def _combine(cols, r0, r1, r2, meta, y_ref, b0, b1, b2, p0, p1, p2, q0, q1, q2, h0, h1, h2, mw, rsem, send, recv):
    me = _where()
    z, y, x, c = me
    R, B, S, Q, H = (r0, r1, r2), (b0, b1, b2), (p0, p1, p2), (q0, q1, q2), (h0, h1, h2)
    axis = (z, y, x)
    T = y_ref.shape[0]
    C = b0.shape[2]
    L = 2 * N * C
    h = T // 2
    halves = (pl.ds(0, h), pl.ds(h, h))
    for p in range(3):
        for k in (2, 1, 3, 0):
            a = (axis[p] + k) % N
            pltpu.make_async_copy(R[p].at[a], B[p].at[a], rsem.at[p, k]).start()

    def partial(p, k):
        a = (axis[p] + k) % N
        _wait(B[p].at[0], rsem.at[p, k])

        @pl.loop(0, N)
        def _(b):
            row = (z * N + b, b * N + y, b * N + x)[p]
            tab = meta[p, a, 0, pl.ds(row, 1), :]
            g = meta[p, a, 1, pl.ds(row, 1), :]
            hot = lax.broadcasted_iota(jnp.int32, (T, L), 0).astype(F32) == tab
            m = jnp.where(hot, g, 0.0)
            here = pl.ds(pl.multiple_of(b * L, L), L)
            for q in range(3):
                part = m.astype(BF16)
                mw[q * T:(q + 1) * T, here] = part
                m = m - part.astype(F32)

        v = B[p][a].reshape(N * L, cols[p][1])
        t = jnp.dot(mw[...], v, preferred_element_type=F32)
        S[p][k] = t[:T] + t[T:2 * T] + t[2 * T:]

    def side(p, k):
        return _along(p, me, (axis[p] + (1, 3)[k]) % N)

    for p in range(3):
        partial(p, 2)
        for k in range(2):
            _copy(S[p].at[2, halves[k]], H[p].at[k], send.at[p, k], recv.at[p, k], side(p, k)).start()
    for p in range(3):
        for k in range(2):
            partial(p, (1, 3)[k])
            _wait(H[p].at[k], recv.at[p, k])
            S[p][(1, 3)[k], halves[k]] += H[p][k]
            _copy(S[p].at[(1, 3)[k]], Q[p].at[k], send.at[p, 2 + k], recv.at[p, 2 + k], side(p, k)).start()
    for p in range(3):
        partial(p, 0)
    for p in range(3):
        t = S[p][0]
        for k in range(2):
            _wait(Q[p].at[k], recv.at[p, 2 + k])
            t += Q[p][k]
        y_ref[:, pl.ds(*cols[p])] = t.astype(BF16)
    for p in range(3):
        for k in range(2):
            _wait(H[p].at[k], send.at[p, k])
            _wait(Q[p].at[k], send.at[p, 2 + k])


def _plan(x, wr, idx, cap):
    T = x.shape[0]
    E = wr.shape[1]
    logits = jnp.dot(x, wr, preferred_element_type=F32)
    oh = idx[:, :, None] == jnp.arange(E, dtype=idx.dtype)
    g = jax.nn.softmax(jnp.sum(jnp.where(oh, logits[:, None, :], 0.0), axis=-1), axis=-1)
    m = jnp.sum(oh, axis=1, dtype=jnp.int32).astype(F32)
    ge = jnp.sum(jnp.where(oh, g[:, :, None], 0.0), axis=1)
    pos = jnp.arange(T, dtype=jnp.int32)
    tri = (pos[None, :] < pos[:, None]).astype(BF16)
    cnt = jnp.dot(tri, m.astype(BF16), preferred_element_type=F32)
    cnt = jnp.where(m > 0, cnt, -1.0)
    hit = cnt[:, :, None] == jnp.arange(cap, dtype=F32)
    tab = jnp.sum(jnp.where(hit, pos.astype(F32)[:, None, None] + 1.0, 0.0), axis=0) - 1.0
    gw = jnp.sum(jnp.where(hit, ge[:, :, None], 0.0), axis=0)

    def both(v):
        v = v.reshape(N, N, N, 2 * cap)
        return v.reshape(N * N, 2 * N * cap), v.transpose(0, 2, 1, 3).reshape(N * N, 2 * N * cap)

    (t0, t2), (g0, g2) = both(tab), both(gw)
    return jnp.stack([jnp.stack([t0, g0]), jnp.stack([t2, g2])])


def solution(mesh):
    assert (mesh.shape['outer'], mesh.shape['expert']) == (N * N, 2 * N)
    tok = P(('data', 'outer', 'expert'), None)
    wsp = P(('outer', 'expert'), None, None)
    any_ = pl.BlockSpec(memory_space=pl.ANY)
    vmem = pl.BlockSpec(memory_space=pltpu.VMEM)
    dma = pltpu.SemaphoreType.DMA
    params = pltpu.CompilerParams(has_side_effects=True, vmem_limit_bytes=60 * 1024 * 1024)

    def local(x, wr, idx, w1, w3, w2):
        T, D = x.shape
        E = wr.shape[1]
        C = 2 * T * idx.shape[1] // E
        ff = w1.shape[2]
        cols = _cols(D)
        widths = [w for _, w in cols]
        L = 2 * N * C
        K = 2 * N * N
        blocks = [(N, K, C, w) for w in widths]
        held = [pltpu.VMEM(b, BF16) for b in blocks]
        meta = _plan(x, wr, idx, C)
        xin, metas = pl.pallas_call(
            functools.partial(_dispatch, cols),
            name='dispatch',
            out_shape=[jax.ShapeDtypeStruct((N, N, N, 2, C, D), BF16), jax.ShapeDtypeStruct((3, N, 2, N * N, L), F32)],
            in_specs=[any_, any_],
            out_specs=[any_, vmem],
            scratch_shapes=[pltpu.VMEM((N, T, w), BF16) for w in widths] + [pltpu.VMEM((3, N, 2, N * N, L), F32)] + held + held
            + [dma((3,)), dma((3, 2)), dma((3, 4)), dma((3, 4)), dma((3, 4)), dma((3, 4)), dma((3,)), dma((3,)), dma((3,)), dma((3, K)), dma((3,))],
            compiler_params=params,
        )(x, meta)
        r = pl.pallas_call(
            functools.partial(_experts, cols),
            name='experts',
            out_shape=[jax.ShapeDtypeStruct(b, BF16) for b in blocks],
            in_specs=[any_] * 4,
            out_specs=[any_] * 3,
            scratch_shapes=[
                pltpu.VMEM((D, ff), BF16), pltpu.VMEM((D, ff), BF16), pltpu.VMEM((ff, D), BF16),
                pltpu.VMEM((2, 2, N, 2, C, D), BF16), pltpu.VMEM((2 * L, ff), BF16), pltpu.VMEM((N, N, N, 2, C, D), BF16), *held,
                dma((3,)), dma((2, 2)), dma((3,)), dma((3,)), dma((3,)), dma((3,)), dma((3, K)), dma((3,)),
            ],
            compiler_params=params,
        )(xin, w1, w3, w2)
        return pl.pallas_call(
            functools.partial(_combine, cols),
            name='combine',
            out_shape=jax.ShapeDtypeStruct((T, D), BF16),
            in_specs=[any_] * 3 + [vmem],
            out_specs=vmem,
            scratch_shapes=held + [pltpu.VMEM((N, T, w), F32) for w in widths] + [pltpu.VMEM((2, T, w), F32) for w in widths]
            + [pltpu.VMEM((2, T // 2, w), F32) for w in widths] + [pltpu.VMEM((3 * T, N * L), BF16), dma((3, N)), dma((3, 4)), dma((3, 4))],
            compiler_params=params,
        )(*r, metas)

    return jax.shard_map(local, mesh=mesh, in_specs=(tok, P(None, None), tok, wsp, wsp, wsp), out_specs=tok, check_vma=False)
```

```python
import functools

import jax
import jax.numpy as jnp
from jax import lax
from jax.experimental import pallas as pl
from jax.experimental.pallas import tpu as pltpu
from jax.sharding import PartitionSpec as P

MESH = pl.DeviceIdType.MESH
F32 = jnp.float32
BF16 = jnp.bfloat16
N = 4


def _cols(d):
    t = d // 128
    w = [(t // 3) * 128, (t // 3) * 128, (t - 2 * (t // 3)) * 128]
    return [(0, w[0]), (w[0], w[1]), (w[0] + w[1], w[2])]


def _where():
    o, e = lax.axis_index('outer'), lax.axis_index('expert')
    return o // N, o % N, e // 2, e % 2


def _dev(z, y, x, c):
    return (0, z * N + y, x * 2 + c)


def _along(p, me, a):
    z, y, x, c = me
    return _dev(*((a, y, x, c), (z, a, x, c), (z, y, a, c))[p])


def _plane(p, me, b, d, c):
    z, y, x, _ = me
    return _dev(*((z, b, d, c), (b, y, d, c), (b, d, x, c))[p])


def _copy(src, dst, send, recv, dev):
    return pltpu.make_async_remote_copy(src_ref=src, dst_ref=dst, send_sem=send, recv_sem=recv, device_id=dev, device_id_type=MESH)


def _wait(ref, sem):
    pltpu.make_async_copy(ref, ref, sem).wait()


def _hops(o):
    return o - 2 * (o // 3)


def _step(o, s):
    return (o + N - s * (o // 2) * (1 - o // 3)) % N


def _order(p, a, b, d):
    return ((a, b, d), (d, a, b), (b, d, a))[p]


def _dispatch(cols, x_ref, rows_ref, meta_ref, xin, meta_out, ag0, ag1, ag2, mt, mb, sb0, sb1, sb2, rl0, rl1, rl2,
              own, lown, asend, arecv, bsend, brecv, tsend, trecv, msend, mrecv, lsend, send, fsend, rrecv, recv):
    me = _where()
    z, y, x, c = me
    ag, sb, rl = (ag0, ag1, ag2), (sb0, sb1, sb2), (rl0, rl1, rl2)
    T = x_ref.shape[0]
    C = sb0.shape[3]
    L = 2 * N * C
    h = T // 2
    axis = (z, y, x)
    base = ((z, y, x), (y, x, z), (x, z, y))
    which = (0, 0, 1)
    parts = range(3)
    sides = (1, 3)
    halves = (pl.ds(0, h), pl.ds(h, h))

    def to_a(p, k):
        a, b, d = base[p]
        return _dev(*_order(p, (a + k) % N, b, d), c)

    def to_b(p, k):
        a, b, d = base[p]
        return _dev(*_order(p, a, (b + k) % N, d), c)

    def give_b(p, k, src):
        a, b, d = base[p]
        for q in range(2):
            _copy(src, ag[p].at[(a + k) % N, b], bsend.at[p, q, k], brecv.at[p, q, k], to_b(p, sides[q])).start()

    def pass_b(p, k):
        a, b, d = base[p]
        for q in range(2):
            _wait(ag[p].at[0, 0], brecv.at[p, q, k])
            blk = ag[p].at[(a + k) % N, (b + (3, 1)[q]) % N, halves[q]]
            _copy(blk, blk, bsend.at[p, 2 + q, k], brecv.at[p, 2 + q, k], to_b(p, sides[q])).start()

    for p in parts:
        a, b, d = base[p]
        blk = x_ref.at[:, pl.ds(*cols[p])]
        for q in range(2):
            _copy(blk, ag[p].at[a, b], asend.at[p, q], arecv.at[p, q], to_a(p, sides[q])).start()
        pltpu.make_async_copy(blk, ag[p].at[a, b], lown.at[p, 0]).start()
    for p in parts:
        a, b, d = base[p]
        for ka in range(N):
            for kb in range(N):
                at = _dev(*_order(p, (a + ka) % N, (b + kb) % N, d), c)
                src = rows_ref.at[p, (a + ka) % N * N + (b + kb) % N]
                if ka + kb:
                    _copy(src, mt.at[p, a, b], tsend.at[p], trecv.at[p], at).start()
                else:
                    pltpu.make_async_copy(src, mt.at[p, a, b], lown.at[p, 1]).start()
    for p in parts:
        give_b(p, 0, x_ref.at[:, pl.ds(*cols[p])])
    for p in parts:
        a, b, d = base[p]
        for q in range(2):
            _wait(ag[p].at[0, 0], arecv.at[p, q])
            blk = ag[p].at[(a + (3, 1)[q]) % N, b, halves[q]]
            _copy(blk, blk, asend.at[p, 2 + q], arecv.at[p, 2 + q], to_a(p, sides[q])).start()
    for p in parts:
        a, b, d = base[p]
        for k in sides:
            give_b(p, k, ag[p].at[(a + k) % N, b])
    for p in parts:
        for k in (1, 3, 2):
            _copy(meta_ref.at[which[p]], mb.at[p, axis[p]], msend.at[p, k], mrecv.at[p, k], _along(p, me, (axis[p] + k) % N)).start()
        pltpu.make_async_copy(meta_ref.at[which[p]], mb.at[p, axis[p]], lown.at[p, 2]).start()
    for p in parts:
        pass_b(p, 0)
    for p in parts:
        a, b, d = base[p]
        for q in range(2):
            _wait(ag[p].at[0, 0, halves[q]], arecv.at[p, 2 + q])
        give_b(p, 2, ag[p].at[(a + 2) % N, b])
        _wait(ag[p].at[0, 0], lown.at[p, 0])
        _wait(mt.at[p, 0, 0], lown.at[p, 1])
        _wait(rows_ref.at[p, pl.ds(0, N * N - 1)], trecv.at[p])

    def final(p, bs, ds):
        i = _order(p, slice(None), bs, ds)
        return xin.at[i[0], i[1], i[2], c, :, pl.ds(*cols[p])]

    def select(p, bo):
        a_, b, d = base[p]
        w = cols[p][1]
        bs = (b + bo) % N

        @pl.loop(0, N)
        def _(a):
            hot = lax.broadcasted_iota(jnp.int32, (T, L), 0).astype(F32) == mt[p, a, bs, 0:1, :]
            hot = jnp.where(hot, 1.0, 0.0).astype(BF16)
            r = lax.dot_general(hot, ag[p][a, bs], (((0,), (0,)), ((), ())), preferred_element_type=F32)
            sb[p][a, bo] = r.astype(BF16).reshape(2 * N, C, w)

        for do in (2, 1, 3, 0):
            for cc in range(2):
                s = 1 - 2 * cc
                src = sb[p].at[:, bo, (d + do) % N * 2 + (c + cc) % 2]
                if do == 2:
                    to = _dev(*_order(p, a_, b, (d + N + s) % N), c)
                    _copy(src, rl[p].at[bo, cc], lsend.at[p], rrecv.at[p, bo, cc], to).start()
                elif do + cc:
                    to = _dev(*_order(p, a_, b, (d + do) % N), (c + cc) % 2)
                    _copy(src, final(p, bs, d), send.at[p], recv.at[p], to).start()
                else:
                    pltpu.make_async_copy(src, final(p, bs, d), own.at[p]).start()

    def relay(p, bo):
        a, b, d = base[p]
        for cc in range(2):
            s = 1 - 2 * cc
            _wait(rl[p].at[bo, cc], rrecv.at[p, bo, cc])
            to = _dev(*_order(p, a, b, (d + N + s) % N), (c + cc) % 2)
            _copy(rl[p].at[bo, cc], final(p, (b + bo) % N, (d + N - s) % N), fsend.at[p], recv.at[p], to).start()

    for p in parts:
        select(p, 0)
        for k in sides:
            pass_b(p, k)
    for p in parts:
        pass_b(p, 2)
        for bo in sides:
            select(p, bo)
        relay(p, 0)
    for p in parts:
        for k in range(N):
            for q in range(2):
                _wait(ag[p].at[0, 0, halves[q]], brecv.at[p, 2 + q, k])
        select(p, 2)
        for bo in sides:
            relay(p, bo)
    for p in parts:
        relay(p, 2)
    for p in parts:
        _wait(mb.at[p, 0], lown.at[p, 2])
        for k in (1, 2, 3):
            _wait(mb.at[p, 0], mrecv.at[p, k])
    meta_out[...] = mb[...]
    for p in parts:
        for k in (1, 2, 3):
            _wait(mb.at[p, 0], msend.at[p, k])
        _wait(rows_ref.at[p, pl.ds(0, N * N - 1)], tsend.at[p])
        for q in range(2):
            _wait(ag[p].at[0, 0], asend.at[p, q])
            _wait(ag[p].at[0, 0, halves[q]], asend.at[p, 2 + q])
            for k in range(N):
                _wait(ag[p].at[0, 0], bsend.at[p, q, k])
                _wait(ag[p].at[0, 0, halves[q]], bsend.at[p, 2 + q, k])
        _wait(sb[p].at[:, :, 0], own.at[p])
        _wait(sb[p].at[:, :, pl.ds(0, 2)], fsend.at[p])
        _wait(sb[p].at[:, :, pl.ds(0, 2)], lsend.at[p])
        _wait(sb[p].at[:, :, pl.ds(0, 5)], send.at[p])
        _wait(sb[p].at[:, :, pl.ds(0, 7)], recv.at[p])


FIRST_B = (False, True, False)


def _bd(p, f, g):
    return (f, g) if FIRST_B[p] else (g, f)


def _spot(fo, go, cc, r):
    s = 1 - 2 * cc
    nf = min(r, _hops(fo))
    ng = r - nf
    return (N + {0: 0, 1: 1, 2: s, 3: -1}[fo] * nf) % N, (N + {0: 0, 1: 1, 2: s, 3: -1}[go] * ng) % N


WAYS = [(fo, go, cc) for fo in (2, 1, 3, 0) for go in (2, 1, 3, 0) for cc in range(2)]
LATER = [(k, r) for r in (2, 3) for k in WAYS if _hops(k[0]) + _hops(k[1]) > r]
ONCE = [k for k in WAYS if _hops(k[0]) + _hops(k[1]) > 1]
NEAR = 2 * N * N - len(ONCE) - 1


def _experts(cols, xin, w1_ref, w3_ref, w2_ref, r0, r1, r2, w1, w3, w2, xb, hb, ob, rl0, rl1, rl2, rm0, rm1, rm2,
             wsem, xsem, own, lsend, send, fsend, isend, rrecv, irecv, recv):
    me = _where()
    z, y, x, c = me
    R, rl, rm = (r0, r1, r2), (rl0, rl1, rl2), (rm0, rm1, rm2)
    C, D = xin.shape[4:]
    G = 2 * N * C
    ff = w1.shape[1]
    half = N // 2
    steps = N * half
    base = ((y, x), (z, x), (z, y))
    loads = [pltpu.make_async_copy(s.at[0], d, wsem.at[q]) for q, (s, d) in enumerate(((w1_ref, w1), (w3_ref, w3), (w2_ref, w2)))]

    def place(s):
        zo = (2 + 3 * (s // half)) % N
        yo = [(2 + 2 * (s % half) + 3 * q) % N for q in range(2)]
        return (z + zo) % N, zo, [(y + o) % N for o in yo], yo

    def load(s):
        zt, _, ys, _ = place(s)
        return [pltpu.make_async_copy(xin.at[zt, yv], xb.at[s % 2, q], xsem.at[s % 2, q]) for q, yv in enumerate(ys)]

    for q in load(0):
        q.start()
    for q in loads:
        q.start()
    cs = [pl.ds(lo, w) for lo, w in cols]

    def at(p, f, g, cc):
        bo, do = _bd(p, f, g)
        return _plane(p, me, (base[p][0] + bo) % N, (base[p][1] + do) % N, (c + cc) % 2)

    def put(p, src, fo, go, cc, lead):
        s = 1 - 2 * cc
        key = (fo * N + go) * 2 + cc
        n = _hops(fo) + _hops(go)
        hf, hg = _step(fo, s), (1 - (fo + N - 1) // N) * _step(go, s)
        dst = R[p].at[lead, (base[p][0] * N + base[p][1]) * 2 + c]
        leg = _copy(src, rl[p].at[lead, key], lsend.at[p], rrecv.at[p, key], at(p, hf, hg, 0))
        far = _copy(src, dst, send.at[p], recv.at[p], at(p, hf, hg, cc))

        @pl.when(n > 1)
        def _():
            leg.start()

        if cc:
            @pl.when(n < 2)
            def _():
                far.start()
        else:
            @pl.when(n == 1)
            def _():
                far.start()

            @pl.when(n == 0)
            def _():
                pltpu.make_async_copy(src, dst, own.at[p]).start()

    fs, ds = min(256, ff), min(512, D)
    every = slice(None)

    @pl.loop(0, steps)
    def _(s):
        zt, zo, ys, yo = place(s)
        jp = s % half

        @pl.when(s + 1 < steps)
        def _():
            for q in load(s + 1):
                q.start()

        for q in load(s):
            q.wait()

        @pl.when(s == 0)
        def _():
            for q in loads:
                q.wait()

        @pl.loop(0, ff // fs)
        def _(f):
            fc = pl.ds(pl.multiple_of(f * fs, fs), fs)
            xt = xb[s % 2].reshape(2 * G, D)
            a = jnp.dot(xt, w1[:, fc], preferred_element_type=F32)
            b = jnp.dot(xt, w3[:, fc], preferred_element_type=F32)
            hb[:, fc] = (jax.nn.silu(a) * b).astype(BF16)

        @pl.loop(0, D // ds)
        def _(f):
            fc = pl.ds(pl.multiple_of(f * ds, ds), ds)
            o = jnp.dot(hb[...], w2[:, fc], preferred_element_type=F32).astype(BF16)
            ob[zt, ys[0], :, :, :, fc] = o[:G].reshape(N, 2, C, ds)
            ob[zt, ys[1], :, :, :, fc] = o[G:].reshape(N, 2, C, ds)

        for q in range(2):
            for cc in range(2):
                put(2, ob.at[zt, ys[q], :, (c + cc) % 2, :, cs[2]], yo[q], zo, cc, every)

            @pl.loop(0, N)
            def _(j):
                do = (2 + 3 * j) % N
                for cc in range(2):
                    put(0, ob.at[zt, ys[q], (x + do) % N, (c + cc) % 2, :, cs[0]], do, yo[q], cc, zt)

        @pl.when(jp == half - 1)
        def _():
            @pl.loop(0, N)
            def _(j):
                do = (2 + 3 * j) % N
                for cc in range(2):
                    put(1, ob.at[zt, :, (x + do) % N, (c + cc) % 2, :, cs[1]], zo, do, cc, every)

    def forward(p, key, r):
        fo, go, cc = key
        here, there = _spot(fo, go, cc, r), _spot(fo, go, cc, r + 1)
        k = (fo * N + go) * 2 + cc
        if r == 1:
            buf, sem = rl[p].at[:, k], rrecv.at[p, k]
        else:
            k = LATER.index((key, r))
            buf, sem = rm[p].at[:, k], irecv.at[p, k]
        _wait(buf, sem)
        hop = [(there[q] + N - here[q]) % N for q in range(2)]
        if r + 1 == _hops(fo) + _hops(go):
            bs, ds = ((base[p][q] + N - v) % N for q, v in enumerate(_bd(p, *here)))
            _copy(buf, R[p].at[:, (bs * N + ds) * 2 + c], fsend.at[p], recv.at[p], at(p, *hop, cc)).start()
        else:
            k = LATER.index((key, r + 1))
            _copy(buf, rm[p].at[:, k], isend.at[p], irecv.at[p, k], at(p, *hop, 0)).start()

    for long in (True, False):
        for key in ONCE:
            if (_hops(key[0]) + _hops(key[1]) > 2) == long:
                for p in (2, 1, 0):
                    forward(p, key, 1)
    for key, r in LATER:
        for p in (2, 1, 0):
            forward(p, key, r)
    for p in range(3):
        _wait(R[p].at[:, 0], own.at[p])
        _wait(R[p].at[:, pl.ds(0, NEAR)], send.at[p])
        _wait(R[p].at[:, pl.ds(0, len(ONCE))], lsend.at[p])
        _wait(R[p].at[:, pl.ds(0, len(ONCE))], fsend.at[p])
        _wait(R[p].at[:, pl.ds(0, len(LATER))], isend.at[p])
        _wait(R[p].at[:, pl.ds(0, 2 * N * N - 1)], recv.at[p])


def _combine(cols, r0, r1, r2, meta, y_ref, b0, b1, b2, p0, p1, p2, q0, q1, q2, h0, h1, h2, mw, rsem, send, recv):
    me = _where()
    z, y, x, c = me
    R, B, S, Q, H = (r0, r1, r2), (b0, b1, b2), (p0, p1, p2), (q0, q1, q2), (h0, h1, h2)
    axis = (z, y, x)
    T = y_ref.shape[0]
    C = b0.shape[2]
    L = 2 * N * C
    h = T // 2
    halves = (pl.ds(0, h), pl.ds(h, h))
    for p in range(3):
        for k in (2, 1, 3, 0):
            a = (axis[p] + k) % N
            pltpu.make_async_copy(R[p].at[a], B[p].at[a], rsem.at[p, k]).start()

    def partial(p, k):
        a = (axis[p] + k) % N
        _wait(B[p].at[0], rsem.at[p, k])

        @pl.loop(0, N)
        def _(b):
            row = (z * N + b, b * N + y, b * N + x)[p]
            tab = meta[p, a, 0, pl.ds(row, 1), :]
            g = meta[p, a, 1, pl.ds(row, 1), :]
            hot = lax.broadcasted_iota(jnp.int32, (T, L), 0).astype(F32) == tab
            m = jnp.where(hot, g, 0.0)
            here = pl.ds(pl.multiple_of(b * L, L), L)
            for q in range(3):
                part = m.astype(BF16)
                mw[q * T:(q + 1) * T, here] = part
                m = m - part.astype(F32)

        v = B[p][a].reshape(N * L, cols[p][1])
        t = jnp.dot(mw[...], v, preferred_element_type=F32)
        S[p][k] = t[:T] + t[T:2 * T] + t[2 * T:]

    def side(p, k):
        return _along(p, me, (axis[p] + (1, 3)[k]) % N)

    for p in range(3):
        partial(p, 2)
        for k in range(2):
            _copy(S[p].at[2, halves[k]], H[p].at[k], send.at[p, k], recv.at[p, k], side(p, k)).start()
    for p in range(3):
        for k in range(2):
            partial(p, (1, 3)[k])
            _wait(H[p].at[k], recv.at[p, k])
            S[p][(1, 3)[k], halves[k]] += H[p][k]
            _copy(S[p].at[(1, 3)[k]], Q[p].at[k], send.at[p, 2 + k], recv.at[p, 2 + k], side(p, k)).start()
    for p in range(3):
        partial(p, 0)
    for p in range(3):
        t = S[p][0]
        for k in range(2):
            _wait(Q[p].at[k], recv.at[p, 2 + k])
            t += Q[p][k]
        y_ref[:, pl.ds(*cols[p])] = t.astype(BF16)
    for p in range(3):
        for k in range(2):
            _wait(H[p].at[k], send.at[p, k])
            _wait(Q[p].at[k], send.at[p, 2 + k])


def _plan(x, wr, idx, cap):
    T = x.shape[0]
    E = wr.shape[1]
    logits = jnp.dot(x, wr, preferred_element_type=F32)
    oh = idx[:, :, None] == jnp.arange(E, dtype=idx.dtype)
    g = jax.nn.softmax(jnp.sum(jnp.where(oh, logits[:, None, :], 0.0), axis=-1), axis=-1)
    m = jnp.sum(oh, axis=1, dtype=jnp.int32).astype(F32)
    ge = jnp.sum(jnp.where(oh, g[:, :, None], 0.0), axis=1)
    pos = jnp.arange(T, dtype=jnp.int32)
    tri = (pos[None, :] < pos[:, None]).astype(BF16)
    cnt = jnp.dot(tri, m.astype(BF16), preferred_element_type=F32)
    cnt = jnp.where(m > 0, cnt, -1.0)
    hit = cnt[:, :, None] == jnp.arange(cap, dtype=F32)
    tab = jnp.sum(jnp.where(hit, pos.astype(F32)[:, None, None] + 1.0, 0.0), axis=0) - 1.0
    gw = jnp.sum(jnp.where(hit, ge[:, :, None], 0.0), axis=0)

    def both(v):
        v = v.reshape(N, N, N, 2 * cap)
        return v.reshape(N * N, 2 * N * cap), v.transpose(0, 2, 1, 3).reshape(N * N, 2 * N * cap)

    (t0, t2), (g0, g2) = both(tab), both(gw)
    t = tab.reshape(N, N, N, 2 * cap)
    rows = jnp.stack([t, t.transpose(1, 2, 0, 3), t.transpose(2, 0, 1, 3)]).reshape(3, N * N, 1, 2 * N * cap)
    return jnp.broadcast_to(rows, (3, N * N, 8, 2 * N * cap)), jnp.stack([jnp.stack([t0, g0]), jnp.stack([t2, g2])])


def solution(mesh):
    assert (mesh.shape['outer'], mesh.shape['expert']) == (N * N, 2 * N)
    tok = P(('data', 'outer', 'expert'), None)
    wsp = P(('outer', 'expert'), None, None)
    any_ = pl.BlockSpec(memory_space=pl.ANY)
    vmem = pl.BlockSpec(memory_space=pltpu.VMEM)
    dma = pltpu.SemaphoreType.DMA
    params = pltpu.CompilerParams(has_side_effects=True, vmem_limit_bytes=63 * 1024 * 1024)

    def local(x, wr, idx, w1, w3, w2):
        T, D = x.shape
        E = wr.shape[1]
        C = 2 * T * idx.shape[1] // E
        ff = w1.shape[2]
        cols = _cols(D)
        widths = [w for _, w in cols]
        L = 2 * N * C
        K = 2 * N * N
        blocks = [(N, K, C, w) for w in widths]
        held = [pltpu.VMEM(b, BF16) for b in blocks]
        rows, meta = _plan(x, wr, idx, C)
        xin, metas = pl.pallas_call(
            functools.partial(_dispatch, cols),
            name='dispatch',
            out_shape=[jax.ShapeDtypeStruct((N, N, N, 2, C, D), BF16), jax.ShapeDtypeStruct((3, N, 2, N * N, L), F32)],
            in_specs=[any_] * 3,
            out_specs=[any_, vmem],
            scratch_shapes=[pltpu.VMEM((N, N, T, w), BF16) for w in widths]
            + [pltpu.VMEM((3, N, N, 8, L), F32), pltpu.VMEM((3, N, 2, N * N, L), F32)]
            + [pltpu.VMEM((N, N, 2 * N, C, w), BF16) for w in widths] + [pltpu.VMEM((N, 2, N, C, w), BF16) for w in widths]
            + [dma((3,)), dma((3, 3)), dma((3, 4)), dma((3, 4)), dma((3, 4, N)), dma((3, 4, N)), dma((3,)), dma((3,)), dma((3, 4)), dma((3, 4)),
               dma((3,)), dma((3,)), dma((3,)), dma((3, N, 2)), dma((3,))],
            compiler_params=params,
        )(x, rows, meta)
        r = pl.pallas_call(
            functools.partial(_experts, cols),
            name='experts',
            out_shape=[jax.ShapeDtypeStruct(b, BF16) for b in blocks],
            in_specs=[any_] * 4,
            out_specs=[any_] * 3,
            scratch_shapes=[
                pltpu.VMEM((D, ff), BF16), pltpu.VMEM((D, ff), BF16), pltpu.VMEM((ff, D), BF16),
                pltpu.VMEM((2, 2, N, 2, C, D), BF16), pltpu.VMEM((2 * L, ff), BF16), pltpu.VMEM((N, N, N, 2, C, D), BF16), *held,
                *(pltpu.VMEM((N, len(LATER), C, w), BF16) for w in widths),
                dma((3,)), dma((2, 2)), dma((3,)), dma((3,)), dma((3,)), dma((3,)), dma((3,)), dma((3, K)), dma((3, len(LATER))), dma((3,)),
            ],
            compiler_params=params,
        )(xin, w1, w3, w2)
        return pl.pallas_call(
            functools.partial(_combine, cols),
            name='combine',
            out_shape=jax.ShapeDtypeStruct((T, D), BF16),
            in_specs=[any_] * 3 + [vmem],
            out_specs=vmem,
            scratch_shapes=held + [pltpu.VMEM((N, T, w), F32) for w in widths] + [pltpu.VMEM((2, T, w), F32) for w in widths]
            + [pltpu.VMEM((2, T // 2, w), F32) for w in widths] + [pltpu.VMEM((3 * T, N * L), BF16), dma((3, N)), dma((3, 4)), dma((3, 4))],
            compiler_params=params,
        )(*r, metas)

    return jax.shard_map(local, mesh=mesh, in_specs=(tok, P(None, None), tok, wsp, wsp, wsp), out_specs=tok, check_vma=False)
```

```python
import functools

import jax
import jax.numpy as jnp
from jax import lax
from jax.experimental import pallas as pl
from jax.experimental.pallas import tpu as pltpu
from jax.sharding import PartitionSpec as P

MESH = pl.DeviceIdType.MESH
F32 = jnp.float32
BF16 = jnp.bfloat16
N = 4


def _cols(d):
    t = d // 128
    w = [(t // 3) * 128, (t // 3) * 128, (t - 2 * (t // 3)) * 128]
    return [(0, w[0]), (w[0], w[1]), (w[0] + w[1], w[2])]


def _where():
    o, e = lax.axis_index('outer'), lax.axis_index('expert')
    return o // N, o % N, e // 2, e % 2


def _dev(z, y, x, c):
    return (0, z * N + y, x * 2 + c)


def _along(p, me, a):
    z, y, x, c = me
    return _dev(*((a, y, x, c), (z, a, x, c), (z, y, a, c))[p])


def _plane(p, me, b, d, c):
    z, y, x, _ = me
    return _dev(*((z, b, d, c), (b, y, d, c), (b, d, x, c))[p])


def _copy(src, dst, send, recv, dev):
    return pltpu.make_async_remote_copy(src_ref=src, dst_ref=dst, send_sem=send, recv_sem=recv, device_id=dev, device_id_type=MESH)


def _wait(ref, sem):
    pltpu.make_async_copy(ref, ref, sem).wait()


def _hops(o):
    return o - 2 * (o // 3)


def _step(o, s):
    return (o + N - s * (o // 2) * (1 - o // 3)) % N


def _order(p, a, b, d):
    return ((a, b, d), (d, a, b), (b, d, a))[p]


def _dispatch(cols, x_ref, rows_ref, meta_ref, xin, meta_out, ag0, ag1, ag2, mt, mb, sb0, sb1, sb2, rl0, rl1, rl2,
              own, lown, asend, arecv, bsend, brecv, tsend, trecv, msend, mrecv, lsend, send, fsend, rrecv, recv):
    me = _where()
    z, y, x, c = me
    ag, sb, rl = (ag0, ag1, ag2), (sb0, sb1, sb2), (rl0, rl1, rl2)
    T = x_ref.shape[0]
    C = sb0.shape[3]
    L = 2 * N * C
    h = T // 2
    axis = (z, y, x)
    base = ((z, y, x), (y, x, z), (x, z, y))
    which = (0, 0, 1)
    parts = range(3)
    sides = (1, 3)
    halves = (pl.ds(0, h), pl.ds(h, h))

    def to_a(p, k):
        a, b, d = base[p]
        return _dev(*_order(p, (a + k) % N, b, d), c)

    def to_b(p, k):
        a, b, d = base[p]
        return _dev(*_order(p, a, (b + k) % N, d), c)

    def give_b(p, k, src):
        a, b, d = base[p]
        for q in range(2):
            _copy(src, ag[p].at[(a + k) % N, b], bsend.at[p, q, k], brecv.at[p, q, k], to_b(p, sides[q])).start()

    def pass_b(p, k):
        a, b, d = base[p]
        for q in range(2):
            _wait(ag[p].at[0, 0], brecv.at[p, q, k])
            blk = ag[p].at[(a + k) % N, (b + (3, 1)[q]) % N, halves[q]]
            _copy(blk, blk, bsend.at[p, 2 + q, k], brecv.at[p, 2 + q, k], to_b(p, sides[q])).start()

    for p in parts:
        a, b, d = base[p]
        blk = x_ref.at[:, pl.ds(*cols[p])]
        for q in range(2):
            _copy(blk, ag[p].at[a, b], asend.at[p, q], arecv.at[p, q], to_a(p, sides[q])).start()
        pltpu.make_async_copy(blk, ag[p].at[a, b], lown.at[p, 0]).start()
    for p in parts:
        a, b, d = base[p]
        for ka in range(N):
            for kb in range(N):
                at = _dev(*_order(p, (a + ka) % N, (b + kb) % N, d), c)
                src = rows_ref.at[p, (a + ka) % N * N + (b + kb) % N]
                if ka + kb:
                    _copy(src, mt.at[p, a, b], tsend.at[p], trecv.at[p], at).start()
                else:
                    pltpu.make_async_copy(src, mt.at[p, a, b], lown.at[p, 1]).start()
    for p in parts:
        give_b(p, 0, x_ref.at[:, pl.ds(*cols[p])])
    for p in parts:
        a, b, d = base[p]
        for q in range(2):
            _wait(ag[p].at[0, 0], arecv.at[p, q])
            blk = ag[p].at[(a + (3, 1)[q]) % N, b, halves[q]]
            _copy(blk, blk, asend.at[p, 2 + q], arecv.at[p, 2 + q], to_a(p, sides[q])).start()
    for p in parts:
        a, b, d = base[p]
        for k in sides:
            give_b(p, k, ag[p].at[(a + k) % N, b])
    for p in parts:
        for k in (1, 3, 2):
            _copy(meta_ref.at[which[p]], mb.at[p, axis[p]], msend.at[p, k], mrecv.at[p, k], _along(p, me, (axis[p] + k) % N)).start()
        pltpu.make_async_copy(meta_ref.at[which[p]], mb.at[p, axis[p]], lown.at[p, 2]).start()
    for p in parts:
        pass_b(p, 0)
    for p in parts:
        a, b, d = base[p]
        for q in range(2):
            _wait(ag[p].at[0, 0, halves[q]], arecv.at[p, 2 + q])
        give_b(p, 2, ag[p].at[(a + 2) % N, b])
        _wait(ag[p].at[0, 0], lown.at[p, 0])
        _wait(mt.at[p, 0, 0], lown.at[p, 1])
        _wait(rows_ref.at[p, pl.ds(0, N * N - 1)], trecv.at[p])

    def final(p, bs, ds):
        i = _order(p, slice(None), bs, ds)
        return xin.at[i[0], i[1], i[2], c, :, pl.ds(*cols[p])]

    def select(p, bo):
        a_, b, d = base[p]
        w = cols[p][1]
        bs = (b + bo) % N

        @pl.loop(0, N)
        def _(a):
            hot = lax.broadcasted_iota(jnp.int32, (T, L), 0).astype(F32) == mt[p, a, bs, 0:1, :]
            hot = jnp.where(hot, 1.0, 0.0).astype(BF16)
            r = lax.dot_general(hot, ag[p][a, bs], (((0,), (0,)), ((), ())), preferred_element_type=F32)
            sb[p][a, bo] = r.astype(BF16).reshape(2 * N, C, w)

        for do in (2, 1, 3, 0):
            for cc in range(2):
                s = 1 - 2 * cc
                src = sb[p].at[:, bo, (d + do) % N * 2 + (c + cc) % 2]
                if do == 2:
                    to = _dev(*_order(p, a_, b, (d + N + s) % N), c)
                    _copy(src, rl[p].at[bo, cc], lsend.at[p], rrecv.at[p, bo, cc], to).start()
                elif do + cc:
                    to = _dev(*_order(p, a_, b, (d + do) % N), (c + cc) % 2)
                    _copy(src, final(p, bs, d), send.at[p], recv.at[p], to).start()
                else:
                    pltpu.make_async_copy(src, final(p, bs, d), own.at[p]).start()

    def relay(p, bo):
        a, b, d = base[p]
        for cc in range(2):
            s = 1 - 2 * cc
            _wait(rl[p].at[bo, cc], rrecv.at[p, bo, cc])
            to = _dev(*_order(p, a, b, (d + N + s) % N), (c + cc) % 2)
            _copy(rl[p].at[bo, cc], final(p, (b + bo) % N, (d + N - s) % N), fsend.at[p], recv.at[p], to).start()

    for p in parts:
        select(p, 0)
        for k in sides:
            pass_b(p, k)
    for p in parts:
        pass_b(p, 2)
        for bo in sides:
            select(p, bo)
        relay(p, 0)
    for p in parts:
        for k in range(N):
            for q in range(2):
                _wait(ag[p].at[0, 0, halves[q]], brecv.at[p, 2 + q, k])
        select(p, 2)
        for bo in sides:
            relay(p, bo)
    for p in parts:
        relay(p, 2)
    for p in parts:
        _wait(mb.at[p, 0], lown.at[p, 2])
        for k in (1, 2, 3):
            _wait(mb.at[p, 0], mrecv.at[p, k])
    meta_out[...] = mb[...]
    for p in parts:
        for k in (1, 2, 3):
            _wait(mb.at[p, 0], msend.at[p, k])
        _wait(rows_ref.at[p, pl.ds(0, N * N - 1)], tsend.at[p])
        for q in range(2):
            _wait(ag[p].at[0, 0], asend.at[p, q])
            _wait(ag[p].at[0, 0, halves[q]], asend.at[p, 2 + q])
            for k in range(N):
                _wait(ag[p].at[0, 0], bsend.at[p, q, k])
                _wait(ag[p].at[0, 0, halves[q]], bsend.at[p, 2 + q, k])
        _wait(sb[p].at[:, :, 0], own.at[p])
        _wait(sb[p].at[:, :, pl.ds(0, 2)], fsend.at[p])
        _wait(sb[p].at[:, :, pl.ds(0, 2)], lsend.at[p])
        _wait(sb[p].at[:, :, pl.ds(0, 5)], send.at[p])
        _wait(sb[p].at[:, :, pl.ds(0, 7)], recv.at[p])


FIRST_B = (False, True, False)


def _bd(p, f, g):
    return (f, g) if FIRST_B[p] else (g, f)


def _spot(fo, go, cc, r):
    s = 1 - 2 * cc
    nf = min(r, _hops(fo))
    ng = r - nf
    return (N + {0: 0, 1: 1, 2: s, 3: -1}[fo] * nf) % N, (N + {0: 0, 1: 1, 2: s, 3: -1}[go] * ng) % N


WAYS = [(fo, go, cc) for fo in (2, 1, 3, 0) for go in (2, 1, 3, 0) for cc in range(2)]
LATER = [(k, r) for r in (2, 3) for k in WAYS if _hops(k[0]) + _hops(k[1]) > r]
ONCE = [k for k in WAYS if _hops(k[0]) + _hops(k[1]) > 1]
NEAR = 2 * N * N - len(ONCE) - 1

TILES = [((2, 2), (2, 1)), ((2, 3), (2, 0)), ((1, 2), (3, 2)), ((0, 2), (1, 1)),
         ((1, 3), (1, 0)), ((3, 1), (0, 1)), ((3, 3), (3, 0)), ((0, 3), (0, 0))]
LAG = 2


def _messages():
    seen, steps = set(), []
    for tile in TILES:
        out = []
        for zo, yo in tile:
            seen.add((zo, yo))
            for cc in range(2):
                out.append((2, yo, zo, cc))
        for o in dict.fromkeys(v[0] for v in tile):
            if all((o, k) in seen for k in range(N)) and not any(m[0] == 1 and m[1] == o for t in steps for m in t):
                out += [(1, o, do, cc) for do in (2, 1, 3, 0) for cc in range(2)]
        for o in dict.fromkeys(v[1] for v in tile):
            if all((k, o) in seen for k in range(N)) and not any(m[0] == 0 and m[2] == o for t in steps for m in t):
                out += [(0, do, o, cc) for do in (2, 1, 3, 0) for cc in range(2)]
        steps.append(out)
    assert sum(len(t) for t in steps) == 3 * len(WAYS)
    return steps


def _schedule():
    first = _messages()
    left = {}
    for st, out in enumerate(first):
        for m in out:
            n = _hops(m[1]) + _hops(m[2])
            for r in range(1, n):
                left.setdefault(min(st + LAG * r, len(TILES)), []).append((r, (m[0], m[1:], r)))
    return first, [[v for _, v in sorted(left.get(st, []), key=lambda t: t[0])] for st in range(len(TILES) + 1)]


def _pick(values, s):
    return sum(v * (1 - ((s - k) * (s - k) + 63) // 64) for k, v in enumerate(values))


def _experts(cols, xin, w1_ref, w3_ref, w2_ref, meta, y_ref, r0, r1, r2, rm0, rm1, rm2, w1, w3, w2, xb, hb, ob, rl0, rl1, rl2,
             s0, s1, s2, q0, q1, q2, h0, h1, h2,
             wsem, xsem, own, lsend, send, fsend, isend, rrecv, irecv, recv, bsem, ssend, srecv):
    me = _where()
    z, y, x, c = me
    R, rl, rm = (r0, r1, r2), (rl0, rl1, rl2), (rm0, rm1, rm2)
    C, D = xin.shape[4:]
    G = 2 * N * C
    ff = w1.shape[1]
    steps = len(TILES)
    base = ((y, x), (z, x), (z, y))
    axis = (z, y, x)
    first, later = _schedule()
    loads = [pltpu.make_async_copy(s.at[0], d, wsem.at[q]) for q, (s, d) in enumerate(((w1_ref, w1), (w3_ref, w3), (w2_ref, w2)))]

    def cell(st, q):
        zo, yo = TILES[st][q]
        return (z + zo) % N, (y + yo) % N

    def load(st):
        for q in range(2):
            zt, yv = cell(st, q)
            pltpu.make_async_copy(xin.at[zt, yv], xb.at[st % 2, q], xsem.at[st % 2, q]).start()

    load(0)
    for q in loads:
        q.start()
    cs = [pl.ds(lo, w) for lo, w in cols]

    def at(p, f, g, cc):
        bo, do = _bd(p, f, g)
        return _plane(p, me, (base[p][0] + bo) % N, (base[p][1] + do) % N, (c + cc) % 2)

    def slot(p, b, d):
        return R[p].at[:, pl.ds(((b * N + d) * 2 + c) * C, C)]

    def put(p, fo, go, cc):
        bo, do = _bd(p, fo, go)
        b, d, c2 = (base[p][0] + bo) % N, (base[p][1] + do) % N, (c + cc) % 2
        src = (ob.at[:, b, d, c2, :, cs[0]], ob.at[b, :, d, c2, :, cs[1]], ob.at[b, d, :, c2, :, cs[2]])[p]
        n = _hops(fo) + _hops(go)
        if n > 1:
            k = ONCE.index((fo, go, cc))
            _copy(src, rl[p].at[:, k], lsend.at[p], rrecv.at[p, k], at(p, *_spot(fo, go, cc, 1), 0)).start()
        elif n + cc:
            _copy(src, slot(p, *base[p]), send.at[p], recv.at[p], _plane(p, me, b, d, c2)).start()
        else:
            pltpu.make_async_copy(src, slot(p, *base[p]), own.at[p]).start()

    def forward(p, key, r):
        fo, go, cc = key
        here, there = _spot(fo, go, cc, r), _spot(fo, go, cc, r + 1)
        if r == 1:
            k = ONCE.index(key)
            buf, sem = rl[p].at[:, k], rrecv.at[p, k]
        else:
            k = LATER.index((key, r))
            buf, sem = rm[p].at[:, k], irecv.at[p, k]
        _wait(buf, sem)
        hop = [(there[q] + N - here[q]) % N for q in range(2)]
        if r + 1 == _hops(fo) + _hops(go):
            bs, ds = ((base[p][q] + N - v) % N for q, v in enumerate(_bd(p, *here)))
            _copy(buf, slot(p, bs, ds), fsend.at[p], recv.at[p], at(p, *hop, cc)).start()
        else:
            k = LATER.index((key, r + 1))
            _copy(buf, rm[p].at[:, k], isend.at[p], irecv.at[p, k], at(p, *hop, 0)).start()

    fs, ds = min(256, ff), min(512, D)

    @pl.loop(0, steps)
    def _(s):
        zt = [(z + _pick([t[q][0] for t in TILES], s)) % N for q in range(2)]
        yt = [(y + _pick([t[q][1] for t in TILES], s)) % N for q in range(2)]
        for st in range(steps - 1):
            @pl.when(s == st)
            def _():
                load(st + 1)

        for q in range(2):
            _wait(xb.at[0, q], xsem.at[s % 2, q])

        @pl.when(s == 0)
        def _():
            for q in loads:
                q.wait()

        @pl.loop(0, ff // fs)
        def _(f):
            fc = pl.ds(pl.multiple_of(f * fs, fs), fs)
            xt = xb[s % 2].reshape(2 * G, D)
            a = jnp.dot(xt, w1[:, fc], preferred_element_type=F32)
            b = jnp.dot(xt, w3[:, fc], preferred_element_type=F32)
            hb[:, fc] = (jax.nn.silu(a) * b).astype(BF16)

        @pl.loop(0, D // ds)
        def _(f):
            fc = pl.ds(pl.multiple_of(f * ds, ds), ds)
            o = jnp.dot(hb[...], w2[:, fc], preferred_element_type=F32).astype(BF16)
            ob[zt[0], yt[0], :, :, :, fc] = o[:G].reshape(N, 2, C, ds)
            ob[zt[1], yt[1], :, :, :, fc] = o[G:].reshape(N, 2, C, ds)

        for st in range(steps):
            @pl.when(s == st)
            def _():
                for m in first[st]:
                    put(*m)
                for v in later[st]:
                    forward(*v)

    S, Q, H = (s0, s1, s2), (q0, q1, q2), (h0, h1, h2)
    T = y_ref.shape[0]
    L = 2 * N * C
    h = T // 2
    halves = (pl.ds(0, h), pl.ds(h, h))
    sides = (1, 3)

    def room(k, p):
        return (w1, w3)[k // 2].at[pl.ds(k % 2 * N * L, N * L), pl.ds(0, cols[p][1])]

    def gather(p):
        _wait(slot(p, 0, 0), own.at[p])
        _wait(R[p].at[:, pl.ds(0, (2 * N * N - 1) * C)], recv.at[p])
        for k in (2, 1, 3, 0):
            pltpu.make_async_copy(R[p].at[(axis[p] + k) % N], room(k, p), bsem.at[k]).start()

    def partial(p, k):
        a = (axis[p] + k) % N
        _wait(room(k, p), bsem.at[k])

        @pl.loop(0, N)
        def _(b):
            row = (z * N + b, b * N + y, b * N + x)[p]
            tab = meta[p, a, 0, pl.ds(row, 1), :]
            g = meta[p, a, 1, pl.ds(row, 1), :]
            hot = lax.broadcasted_iota(jnp.int32, (T, L), 0).astype(F32) == tab
            m = jnp.where(hot, g, 0.0)
            here = pl.ds(pl.multiple_of(b * L, L), L)
            for q in range(3):
                part = m.astype(BF16)
                w2[q * T:(q + 1) * T, here] = part
                m = m - part.astype(F32)

        t = jnp.dot(w2[:, pl.ds(0, N * L)], room(k, p)[...], preferred_element_type=F32)
        S[p][k] = t[:T] + t[T:2 * T] + t[2 * T:]

    def side(p, q):
        return _along(p, me, (axis[p] + sides[q]) % N)

    def halfway(p):
        for q in range(2):
            _copy(S[p].at[2, halves[q]], H[p].at[q], ssend.at[p, q], srecv.at[p, q], side(p, q)).start()

    def onward(p):
        for q in range(2):
            _wait(H[p].at[q], srecv.at[p, q])
            S[p][sides[q], halves[q]] += H[p][q]
            _copy(S[p].at[sides[q]], Q[p].at[q], ssend.at[p, 2 + q], srecv.at[p, 2 + q], side(p, q)).start()

    rest = later[steps]
    for v in rest:
        if v[0] == 2 or v[2] == 1:
            forward(*v)
    more = [v for v in rest if not (v[0] == 2 or v[2] == 1)]
    gather(2)
    partial(2, 2)
    halfway(2)
    for v in more:
        if v[2] == 2:
            forward(*v)
    partial(2, 1)
    for v in more:
        if v[2] == 3:
            forward(*v)
    partial(2, 3)
    onward(2)
    partial(2, 0)
    for p in (1, 0):
        gather(p)
        partial(p, 2)
        halfway(p)
        partial(p, 1)
        partial(p, 3)
        onward(p)
        partial(p, 0)
    for p in (2, 1, 0):
        t = S[p][0]
        for q in range(2):
            _wait(Q[p].at[q], srecv.at[p, 2 + q])
            t += Q[p][q]
        y_ref[:, cs[p]] = t.astype(BF16)
    for p in range(3):
        for q in range(2):
            _wait(H[p].at[q], ssend.at[p, q])
            _wait(Q[p].at[q], ssend.at[p, 2 + q])
        _wait(R[p].at[:, pl.ds(0, NEAR * C)], send.at[p])
        _wait(R[p].at[:, pl.ds(0, len(ONCE) * C)], lsend.at[p])
        _wait(R[p].at[:, pl.ds(0, len(ONCE) * C)], fsend.at[p])
        _wait(R[p].at[:, pl.ds(0, len(LATER) * C)], isend.at[p])


def _plan(x, wr, idx, cap):
    T = x.shape[0]
    E = wr.shape[1]
    logits = jnp.dot(x, wr, preferred_element_type=F32)
    oh = idx[:, :, None] == jnp.arange(E, dtype=idx.dtype)
    g = jax.nn.softmax(jnp.sum(jnp.where(oh, logits[:, None, :], 0.0), axis=-1), axis=-1)
    m = jnp.sum(oh, axis=1, dtype=jnp.int32).astype(F32)
    ge = jnp.sum(jnp.where(oh, g[:, :, None], 0.0), axis=1)
    pos = jnp.arange(T, dtype=jnp.int32)
    tri = (pos[None, :] < pos[:, None]).astype(BF16)
    cnt = jnp.dot(tri, m.astype(BF16), preferred_element_type=F32)
    cnt = jnp.where(m > 0, cnt, -1.0)
    hit = cnt[:, :, None] == jnp.arange(cap, dtype=F32)
    tab = jnp.sum(jnp.where(hit, pos.astype(F32)[:, None, None] + 1.0, 0.0), axis=0) - 1.0
    gw = jnp.sum(jnp.where(hit, ge[:, :, None], 0.0), axis=0)

    def both(v):
        v = v.reshape(N, N, N, 2 * cap)
        return v.reshape(N * N, 2 * N * cap), v.transpose(0, 2, 1, 3).reshape(N * N, 2 * N * cap)

    (t0, t2), (g0, g2) = both(tab), both(gw)
    t = tab.reshape(N, N, N, 2 * cap)
    rows = jnp.stack([t, t.transpose(1, 2, 0, 3), t.transpose(2, 0, 1, 3)]).reshape(3, N * N, 1, 2 * N * cap)
    return jnp.broadcast_to(rows, (3, N * N, 8, 2 * N * cap)), jnp.stack([jnp.stack([t0, g0]), jnp.stack([t2, g2])])


def solution(mesh):
    assert (mesh.shape['outer'], mesh.shape['expert']) == (N * N, 2 * N)
    tok = P(('data', 'outer', 'expert'), None)
    wsp = P(('outer', 'expert'), None, None)
    any_ = pl.BlockSpec(memory_space=pl.ANY)
    vmem = pl.BlockSpec(memory_space=pltpu.VMEM)
    dma = pltpu.SemaphoreType.DMA
    params = pltpu.CompilerParams(has_side_effects=True, vmem_limit_bytes=67043328)

    def local(x, wr, idx, w1, w3, w2):
        T, D = x.shape
        E = wr.shape[1]
        C = 2 * T * idx.shape[1] // E
        ff = w1.shape[2]
        cols = _cols(D)
        widths = [w for _, w in cols]
        L = 2 * N * C
        K = 2 * N * N
        rows, meta = _plan(x, wr, idx, C)
        xin, metas = pl.pallas_call(
            functools.partial(_dispatch, cols),
            name='dispatch',
            out_shape=[jax.ShapeDtypeStruct((N, N, N, 2, C, D), BF16), jax.ShapeDtypeStruct((3, N, 2, N * N, L), F32)],
            in_specs=[any_] * 3,
            out_specs=[any_, vmem],
            scratch_shapes=[pltpu.VMEM((N, N, T, w), BF16) for w in widths]
            + [pltpu.VMEM((3, N, N, 8, L), F32), pltpu.VMEM((3, N, 2, N * N, L), F32)]
            + [pltpu.VMEM((N, N, 2 * N, C, w), BF16) for w in widths] + [pltpu.VMEM((N, 2, N, C, w), BF16) for w in widths]
            + [dma((3,)), dma((3, 3)), dma((3, 4)), dma((3, 4)), dma((3, 4, N)), dma((3, 4, N)), dma((3,)), dma((3,)), dma((3, 4)), dma((3, 4)),
               dma((3,)), dma((3,)), dma((3,)), dma((3, N, 2)), dma((3,))],
            compiler_params=params,
        )(x, rows, meta)
        out = pl.pallas_call(
            functools.partial(_experts, cols),
            name='experts',
            out_shape=[jax.ShapeDtypeStruct((T, D), BF16)] + [jax.ShapeDtypeStruct((N, K * C, w), BF16) for w in widths]
            + [jax.ShapeDtypeStruct((N, len(LATER), C, w), BF16) for w in widths],
            in_specs=[any_] * 4 + [vmem],
            out_specs=[vmem] + [any_] * 6,
            scratch_shapes=[
                pltpu.VMEM((D, ff), BF16), pltpu.VMEM((D, ff), BF16), pltpu.VMEM((ff, D), BF16),
                pltpu.VMEM((2, 2, N, 2, C, D), BF16), pltpu.VMEM((2 * L, ff), BF16), pltpu.VMEM((N, N, N, 2, C, D), BF16),
                *(pltpu.VMEM((N, len(ONCE), C, w), BF16) for w in widths),
                *(pltpu.VMEM((N, T, w), F32) for w in widths), *(pltpu.VMEM((2, T, w), F32) for w in widths),
                *(pltpu.VMEM((2, T // 2, w), F32) for w in widths),
                dma((3,)), dma((2, 2)), dma((3,)), dma((3,)), dma((3,)), dma((3,)), dma((3,)), dma((3, len(ONCE))), dma((3, len(LATER))), dma((3,)),
                dma((N,)), dma((3, 4)), dma((3, 4)),
            ],
            compiler_params=params,
        )(xin, w1, w3, w2, metas)
        return out[0]

    return jax.shard_map(local, mesh=mesh, in_specs=(tok, P(None, None), tok, wsp, wsp, wsp), out_specs=tok, check_vma=False)
```

```python
import functools

import jax
import jax.numpy as jnp
from jax import lax
from jax.experimental import pallas as pl
from jax.experimental.pallas import tpu as pltpu
from jax.sharding import PartitionSpec as P

MESH = pl.DeviceIdType.MESH
F32 = jnp.float32
BF16 = jnp.bfloat16
N = 4


def _cols(d):
    t = d // 128
    w = [(t // 3) * 128, (t // 3) * 128, (t - 2 * (t // 3)) * 128]
    return [(0, w[0]), (w[0], w[1]), (w[0] + w[1], w[2])]


def _where():
    o, e = lax.axis_index('outer'), lax.axis_index('expert')
    return o // N, o % N, e // 2, e % 2


def _dev(z, y, x, c):
    return (0, z * N + y, x * 2 + c)


def _along(p, me, a):
    z, y, x, c = me
    return _dev(*((a, y, x, c), (z, a, x, c), (z, y, a, c))[p])


def _plane(p, me, b, d, c):
    z, y, x, _ = me
    return _dev(*((z, b, d, c), (b, y, d, c), (b, d, x, c))[p])


def _copy(src, dst, send, recv, dev):
    return pltpu.make_async_remote_copy(src_ref=src, dst_ref=dst, send_sem=send, recv_sem=recv, device_id=dev, device_id_type=MESH)


def _wait(ref, sem):
    pltpu.make_async_copy(ref, ref, sem).wait()


def _hops(o):
    return o - 2 * (o // 3)


def _step(o, s):
    return (o + N - s * (o // 2) * (1 - o // 3)) % N


def _order(p, a, b, d):
    return ((a, b, d), (d, a, b), (b, d, a))[p]


def _dispatch(cols, x_ref, rows_ref, meta_ref, xin, meta_out, ag0, ag1, ag2, mt, mb, sb0, sb1, sb2, rl0, rl1, rl2,
              own, lown, asend, arecv, bsend, brecv, tsend, trecv, msend, mrecv, lsend, send, fsend, rrecv, recv):
    me = _where()
    z, y, x, c = me
    ag, sb, rl = (ag0, ag1, ag2), (sb0, sb1, sb2), (rl0, rl1, rl2)
    T = x_ref.shape[0]
    C = sb0.shape[3]
    L = 2 * N * C
    h = T // 2
    axis = (z, y, x)
    base = ((z, y, x), (y, x, z), (x, z, y))
    which = (0, 0, 1)
    parts = range(3)
    sides = (1, 3)
    halves = (pl.ds(0, h), pl.ds(h, h))

    def to_a(p, k):
        a, b, d = base[p]
        return _dev(*_order(p, (a + k) % N, b, d), c)

    def to_b(p, k):
        a, b, d = base[p]
        return _dev(*_order(p, a, (b + k) % N, d), c)

    def give_b(p, k, src):
        a, b, d = base[p]
        for q in range(2):
            _copy(src, ag[p].at[(a + k) % N, b], bsend.at[p, q, k], brecv.at[p, q, k], to_b(p, sides[q])).start()

    def pass_b(p, k):
        a, b, d = base[p]
        for q in range(2):
            _wait(ag[p].at[0, 0], brecv.at[p, q, k])
            blk = ag[p].at[(a + k) % N, (b + (3, 1)[q]) % N, halves[q]]
            _copy(blk, blk, bsend.at[p, 2 + q, k], brecv.at[p, 2 + q, k], to_b(p, sides[q])).start()

    for p in parts:
        a, b, d = base[p]
        blk = x_ref.at[:, pl.ds(*cols[p])]
        for q in range(2):
            _copy(blk, ag[p].at[a, b], asend.at[p, q], arecv.at[p, q], to_a(p, sides[q])).start()
        pltpu.make_async_copy(blk, ag[p].at[a, b], lown.at[p, 0]).start()
    for p in parts:
        a, b, d = base[p]
        for ka in range(N):
            for kb in range(N):
                at = _dev(*_order(p, (a + ka) % N, (b + kb) % N, d), c)
                src = rows_ref.at[p, (a + ka) % N * N + (b + kb) % N]
                if ka + kb:
                    _copy(src, mt.at[p, a, b], tsend.at[p], trecv.at[p], at).start()
                else:
                    pltpu.make_async_copy(src, mt.at[p, a, b], lown.at[p, 1]).start()
    for p in parts:
        give_b(p, 0, x_ref.at[:, pl.ds(*cols[p])])
    for p in parts:
        a, b, d = base[p]
        for q in range(2):
            _wait(ag[p].at[0, 0], arecv.at[p, q])
            blk = ag[p].at[(a + (3, 1)[q]) % N, b, halves[q]]
            _copy(blk, blk, asend.at[p, 2 + q], arecv.at[p, 2 + q], to_a(p, sides[q])).start()
    for p in parts:
        a, b, d = base[p]
        for k in sides:
            give_b(p, k, ag[p].at[(a + k) % N, b])
    for p in parts:
        for k in (1, 3, 2):
            _copy(meta_ref.at[which[p]], mb.at[p, axis[p]], msend.at[p, k], mrecv.at[p, k], _along(p, me, (axis[p] + k) % N)).start()
        pltpu.make_async_copy(meta_ref.at[which[p]], mb.at[p, axis[p]], lown.at[p, 2]).start()
    for p in parts:
        pass_b(p, 0)
    for p in parts:
        a, b, d = base[p]
        for q in range(2):
            _wait(ag[p].at[0, 0, halves[q]], arecv.at[p, 2 + q])
        give_b(p, 2, ag[p].at[(a + 2) % N, b])
        _wait(ag[p].at[0, 0], lown.at[p, 0])
        _wait(mt.at[p, 0, 0], lown.at[p, 1])
        _wait(rows_ref.at[p, pl.ds(0, N * N - 1)], trecv.at[p])

    def final(p, bs, ds):
        i = _order(p, slice(None), bs, ds)
        return xin.at[i[0], i[1], i[2], c, :, pl.ds(*cols[p])]

    def select(p, bo):
        a_, b, d = base[p]
        w = cols[p][1]
        bs = (b + bo) % N

        @pl.loop(0, N)
        def _(a):
            hot = lax.broadcasted_iota(jnp.int32, (T, L), 0).astype(F32) == mt[p, a, bs, 0:1, :]
            hot = jnp.where(hot, 1.0, 0.0).astype(BF16)
            r = lax.dot_general(hot, ag[p][a, bs], (((0,), (0,)), ((), ())), preferred_element_type=F32)
            sb[p][a, bo] = r.astype(BF16).reshape(2 * N, C, w)

        for do in (2, 1, 3, 0):
            for cc in range(2):
                s = 1 - 2 * cc
                src = sb[p].at[:, bo, (d + do) % N * 2 + (c + cc) % 2]
                if do == 2:
                    to = _dev(*_order(p, a_, b, (d + N + s) % N), c)
                    _copy(src, rl[p].at[bo, cc], lsend.at[p], rrecv.at[p, bo, cc], to).start()
                elif do + cc:
                    to = _dev(*_order(p, a_, b, (d + do) % N), (c + cc) % 2)
                    _copy(src, final(p, bs, d), send.at[p], recv.at[p], to).start()
                else:
                    pltpu.make_async_copy(src, final(p, bs, d), own.at[p]).start()

    def relay(p, bo):
        a, b, d = base[p]
        for cc in range(2):
            s = 1 - 2 * cc
            _wait(rl[p].at[bo, cc], rrecv.at[p, bo, cc])
            to = _dev(*_order(p, a, b, (d + N + s) % N), (c + cc) % 2)
            _copy(rl[p].at[bo, cc], final(p, (b + bo) % N, (d + N - s) % N), fsend.at[p], recv.at[p], to).start()

    for p in parts:
        select(p, 0)
        for k in sides:
            pass_b(p, k)
    for p in parts:
        pass_b(p, 2)
        for bo in sides:
            select(p, bo)
        relay(p, 0)
    for p in parts:
        for k in range(N):
            for q in range(2):
                _wait(ag[p].at[0, 0, halves[q]], brecv.at[p, 2 + q, k])
        select(p, 2)
        for bo in sides:
            relay(p, bo)
    for p in parts:
        relay(p, 2)
    for p in parts:
        _wait(mb.at[p, 0], lown.at[p, 2])
        for k in (1, 2, 3):
            _wait(mb.at[p, 0], mrecv.at[p, k])
    meta_out[...] = mb[...]
    for p in parts:
        for k in (1, 2, 3):
            _wait(mb.at[p, 0], msend.at[p, k])
        _wait(rows_ref.at[p, pl.ds(0, N * N - 1)], tsend.at[p])
        for q in range(2):
            _wait(ag[p].at[0, 0], asend.at[p, q])
            _wait(ag[p].at[0, 0, halves[q]], asend.at[p, 2 + q])
            for k in range(N):
                _wait(ag[p].at[0, 0], bsend.at[p, q, k])
                _wait(ag[p].at[0, 0, halves[q]], bsend.at[p, 2 + q, k])
        _wait(sb[p].at[:, :, 0], own.at[p])
        _wait(sb[p].at[:, :, pl.ds(0, 2)], fsend.at[p])
        _wait(sb[p].at[:, :, pl.ds(0, 2)], lsend.at[p])
        _wait(sb[p].at[:, :, pl.ds(0, 5)], send.at[p])
        _wait(sb[p].at[:, :, pl.ds(0, 7)], recv.at[p])


FIRST_B = (False, True, False)


def _bd(p, f, g):
    return (f, g) if FIRST_B[p] else (g, f)


def _spot(fo, go, cc, r):
    s = 1 - 2 * cc
    nf = max(r - _hops(go), 0) if cc else min(r, _hops(fo))
    ng = r - nf
    return (N + {0: 0, 1: 1, 2: s, 3: -1}[fo] * nf) % N, (N + {0: 0, 1: 1, 2: s, 3: -1}[go] * ng) % N


WAYS = [(fo, go, cc) for fo in (2, 1, 3, 0) for go in (2, 1, 3, 0) for cc in range(2)]
LATER = [(k, r) for r in (2, 3) for k in WAYS if _hops(k[0]) + _hops(k[1]) > r]
ONCE = [k for k in WAYS if _hops(k[0]) + _hops(k[1]) > 1]
NEAR = 2 * N * N - len(ONCE) - 1

TILES = [((2, 1), (2, 3)), ((1, 2), (3, 2)), ((2, 2), (2, 0)), ((1, 1), (3, 3)),
         ((1, 3), (3, 1)), ((0, 2), (0, 0)), ((1, 0), (3, 0)), ((0, 1), (0, 3))]


def _later(parts, r, hops):
    keys = [k for k in ONCE if _hops(k[0]) + _hops(k[1]) in hops and _hops(k[0]) + _hops(k[1]) > r]
    keys = sorted(keys, key=lambda k: -_hops(k[0]) - _hops(k[1]))
    return [(p, k, r) for k in keys for p in parts]


def _pick(values, s):
    return sum(v * (1 - ((s - k) * (s - k) + 63) // 64) for k, v in enumerate(values))


def _experts(cols, xin, w1_ref, w3_ref, w2_ref, meta, y_ref, r0, r1, r2, rm0, rm1, rm2, w1, w3, w2, xb, hb, ob, rl0, rl1, rl2,
             s0, s1, s2, q0, q1, q2, h0, h1, h2,
             wsem, xsem, own, lsend, send, fsend, isend, rrecv, irecv, recv, bsem, ssend, srecv):
    me = _where()
    z, y, x, c = me
    R, rl, rm = (r0, r1, r2), (rl0, rl1, rl2), (rm0, rm1, rm2)
    C, D = xin.shape[4:]
    G = 2 * N * C
    ff = w1.shape[1]
    steps = len(TILES)
    base = ((y, x), (z, x), (z, y))
    axis = (z, y, x)
    loads = [pltpu.make_async_copy(s.at[0], d, wsem.at[q]) for q, (s, d) in enumerate(((w1_ref, w1), (w3_ref, w3), (w2_ref, w2)))]

    def cell(st, q):
        zo, yo = TILES[st][q]
        return (z + zo) % N, (y + yo) % N

    def load(st):
        for q in range(2):
            zt, yv = cell(st, q)
            pltpu.make_async_copy(xin.at[zt, yv], xb.at[st % 2, q], xsem.at[st % 2, q]).start()

    load(0)
    for q in loads:
        q.start()
    cs = [pl.ds(lo, w) for lo, w in cols]

    def at(p, f, g, cc):
        bo, do = _bd(p, f, g)
        return _plane(p, me, (base[p][0] + bo) % N, (base[p][1] + do) % N, (c + cc) % 2)

    def slot(p, b, d):
        return R[p].at[:, pl.ds(((b * N + d) * 2 + c) * C, C)]

    def put(p, fo, go, cc, lead, src):
        bo, do = _bd(p, fo, go)
        b, d, c2 = (base[p][0] + bo) % N, (base[p][1] + do) % N, (c + cc) % 2
        dst = R[p].at[lead, pl.ds(((base[p][0] * N + base[p][1]) * 2 + c) * C, C)]
        n = _hops(fo) + _hops(go)
        if n > 1:
            k = ONCE.index((fo, go, cc))
            _copy(src, rl[p].at[lead, k], lsend.at[p], rrecv.at[p, k], at(p, *_spot(fo, go, cc, 1), 0)).start()
        elif n + cc:
            _copy(src, dst, send.at[p], recv.at[p], _plane(p, me, b, d, c2)).start()
        else:
            pltpu.make_async_copy(src, dst, own.at[p]).start()

    def give(st):
        for cc in range(2):
            c2 = (c + cc) % 2
            for q in range(2):
                zo, yo = TILES[st][q]
                zt, yv = cell(st, q)
                put(2, yo, zo, cc, slice(None), ob.at[zt, yv, :, c2, :, cs[2]])
        for do in (2, 1, 3, 0):
            x2 = (x + do) % N
            for cc in range(2):
                c2 = (c + cc) % 2
                for q in range(2):
                    zo, yo = TILES[st][q]
                    zt, yv = cell(st, q)
                    put(0, do, yo, cc, zt, ob.at[zt, yv, x2, c2, :, cs[0]])
                    put(1, zo, do, cc, yv, ob.at[zt, yv, x2, c2, :, cs[1]])

    def forward(p, key, r):
        fo, go, cc = key
        here, there = _spot(fo, go, cc, r), _spot(fo, go, cc, r + 1)
        if r == 1:
            k = ONCE.index(key)
            buf, sem = rl[p].at[:, k], rrecv.at[p, k]
        else:
            k = LATER.index((key, r))
            buf, sem = rm[p].at[:, k], irecv.at[p, k]
        _wait(buf, sem)
        hop = [(there[q] + N - here[q]) % N for q in range(2)]
        if r + 1 == _hops(fo) + _hops(go):
            bs, ds = ((base[p][q] + N - v) % N for q, v in enumerate(_bd(p, *here)))
            _copy(buf, slot(p, bs, ds), fsend.at[p], recv.at[p], at(p, *hop, cc)).start()
        else:
            k = LATER.index((key, r + 1))
            _copy(buf, rm[p].at[:, k], isend.at[p], irecv.at[p, k], at(p, *hop, 0)).start()

    fs, ds = min(256, ff), min(512, D)

    @pl.loop(0, steps)
    def _(s):
        zt = [(z + _pick([t[q][0] for t in TILES], s)) % N for q in range(2)]
        yt = [(y + _pick([t[q][1] for t in TILES], s)) % N for q in range(2)]
        for st in range(steps - 1):
            @pl.when(s == st)
            def _():
                load(st + 1)

        for q in range(2):
            _wait(xb.at[0, q], xsem.at[s % 2, q])

        @pl.when(s == 0)
        def _():
            for q in loads:
                q.wait()

        @pl.loop(0, ff // fs)
        def _(f):
            fc = pl.ds(pl.multiple_of(f * fs, fs), fs)
            xt = xb[s % 2].reshape(2 * G, D)
            a = jnp.dot(xt, w1[:, fc], preferred_element_type=F32)
            b = jnp.dot(xt, w3[:, fc], preferred_element_type=F32)
            hb[:, fc] = (jax.nn.silu(a) * b).astype(BF16)

        @pl.loop(0, D // ds)
        def _(f):
            fc = pl.ds(pl.multiple_of(f * ds, ds), ds)
            o = jnp.dot(hb[...], w2[:, fc], preferred_element_type=F32).astype(BF16)
            ob[zt[0], yt[0], :, :, :, fc] = o[:G].reshape(N, 2, C, ds)
            ob[zt[1], yt[1], :, :, :, fc] = o[G:].reshape(N, 2, C, ds)

        for st in range(steps):
            @pl.when(s == st)
            def _():
                give(st)

    S, Q, H = (s0, s1, s2), (q0, q1, q2), (h0, h1, h2)
    T = y_ref.shape[0]
    L = 2 * N * C
    h = T // 2
    halves = (pl.ds(0, h), pl.ds(h, h))
    sides = (1, 3)

    def room(k, p):
        return (w1, w3)[k // 2].at[pl.ds(k % 2 * N * L, N * L), pl.ds(0, cols[p][1])]

    def gather(p):
        _wait(slot(p, 0, 0), own.at[p])
        _wait(R[p].at[:, pl.ds(0, (2 * N * N - 1) * C)], recv.at[p])
        for k in (2, 1, 3, 0):
            pltpu.make_async_copy(R[p].at[(axis[p] + k) % N], room(k, p), bsem.at[k]).start()

    def partial(p, k):
        a = (axis[p] + k) % N
        _wait(room(k, p), bsem.at[k])

        @pl.loop(0, N)
        def _(b):
            row = (z * N + b, b * N + y, b * N + x)[p]
            tab = meta[p, a, 0, pl.ds(row, 1), :]
            g = meta[p, a, 1, pl.ds(row, 1), :]
            hot = lax.broadcasted_iota(jnp.int32, (T, L), 0).astype(F32) == tab
            m = jnp.where(hot, g, 0.0)
            here = pl.ds(pl.multiple_of(b * L, L), L)
            for q in range(3):
                part = m.astype(BF16)
                w2[q * T:(q + 1) * T, here] = part
                m = m - part.astype(F32)

        t = jnp.dot(w2[:, pl.ds(0, N * L)], room(k, p)[...], preferred_element_type=F32)
        S[p][k] = t[:T] + t[T:2 * T] + t[2 * T:]

    def side(p, q):
        return _along(p, me, (axis[p] + sides[q]) % N)

    def halfway(p):
        for q in range(2):
            _copy(S[p].at[2, halves[q]], H[p].at[q], ssend.at[p, q], srecv.at[p, q], side(p, q)).start()

    def onward(p):
        for q in range(2):
            _wait(H[p].at[q], srecv.at[p, q])
            S[p][sides[q], halves[q]] += H[p][q]
            _copy(S[p].at[sides[q]], Q[p].at[q], ssend.at[p, 2 + q], srecv.at[p, 2 + q], side(p, q)).start()

    def onwards(*args):
        for v in _later(*args):
            forward(*v)

    onwards((2,), 1, (2, 3, 4))
    onwards((1, 0), 1, (3, 4))
    onwards((2,), 2, (3, 4))
    onwards((1, 0), 1, (2,))
    onwards((2,), 3, (4,))
    onwards((1, 0), 2, (3, 4))
    gather(2)
    partial(2, 2)
    halfway(2)
    onwards((1, 0), 3, (4,))
    partial(2, 1)
    partial(2, 3)
    onward(2)
    partial(2, 0)
    for p in (1, 0):
        gather(p)
        partial(p, 2)
        halfway(p)
        partial(p, 1)
        partial(p, 3)
        onward(p)
        partial(p, 0)
    for p in (2, 1, 0):
        t = S[p][0]
        for q in range(2):
            _wait(Q[p].at[q], srecv.at[p, 2 + q])
            t += Q[p][q]
        y_ref[:, cs[p]] = t.astype(BF16)
    for p in range(3):
        for q in range(2):
            _wait(H[p].at[q], ssend.at[p, q])
            _wait(Q[p].at[q], ssend.at[p, 2 + q])
        _wait(R[p].at[:, pl.ds(0, NEAR * C)], send.at[p])
        _wait(R[p].at[:, pl.ds(0, len(ONCE) * C)], lsend.at[p])
        _wait(R[p].at[:, pl.ds(0, len(ONCE) * C)], fsend.at[p])
        _wait(R[p].at[:, pl.ds(0, len(LATER) * C)], isend.at[p])


def _plan(x, wr, idx, cap):
    T = x.shape[0]
    E = wr.shape[1]
    logits = jnp.dot(x, wr, preferred_element_type=F32)
    oh = idx[:, :, None] == jnp.arange(E, dtype=idx.dtype)
    g = jax.nn.softmax(jnp.sum(jnp.where(oh, logits[:, None, :], 0.0), axis=-1), axis=-1)
    m = jnp.sum(oh, axis=1, dtype=jnp.int32).astype(F32)
    ge = jnp.sum(jnp.where(oh, g[:, :, None], 0.0), axis=1)
    pos = jnp.arange(T, dtype=jnp.int32)
    tri = (pos[None, :] < pos[:, None]).astype(BF16)
    cnt = jnp.dot(tri, m.astype(BF16), preferred_element_type=F32)
    cnt = jnp.where(m > 0, cnt, -1.0)
    hit = cnt[:, :, None] == jnp.arange(cap, dtype=F32)
    tab = jnp.sum(jnp.where(hit, pos.astype(F32)[:, None, None] + 1.0, 0.0), axis=0) - 1.0
    gw = jnp.sum(jnp.where(hit, ge[:, :, None], 0.0), axis=0)

    def both(v):
        v = v.reshape(N, N, N, 2 * cap)
        return v.reshape(N * N, 2 * N * cap), v.transpose(0, 2, 1, 3).reshape(N * N, 2 * N * cap)

    (t0, t2), (g0, g2) = both(tab), both(gw)
    t = tab.reshape(N, N, N, 2 * cap)
    rows = jnp.stack([t, t.transpose(1, 2, 0, 3), t.transpose(2, 0, 1, 3)]).reshape(3, N * N, 1, 2 * N * cap)
    return jnp.broadcast_to(rows, (3, N * N, 8, 2 * N * cap)), jnp.stack([jnp.stack([t0, g0]), jnp.stack([t2, g2])])


def solution(mesh):
    assert (mesh.shape['outer'], mesh.shape['expert']) == (N * N, 2 * N)
    tok = P(('data', 'outer', 'expert'), None)
    wsp = P(('outer', 'expert'), None, None)
    any_ = pl.BlockSpec(memory_space=pl.ANY)
    vmem = pl.BlockSpec(memory_space=pltpu.VMEM)
    dma = pltpu.SemaphoreType.DMA
    params = pltpu.CompilerParams(has_side_effects=True, vmem_limit_bytes=67043328)

    def local(x, wr, idx, w1, w3, w2):
        T, D = x.shape
        E = wr.shape[1]
        C = 2 * T * idx.shape[1] // E
        ff = w1.shape[2]
        cols = _cols(D)
        widths = [w for _, w in cols]
        L = 2 * N * C
        K = 2 * N * N
        rows, meta = _plan(x, wr, idx, C)
        xin, metas = pl.pallas_call(
            functools.partial(_dispatch, cols),
            name='dispatch',
            out_shape=[jax.ShapeDtypeStruct((N, N, N, 2, C, D), BF16), jax.ShapeDtypeStruct((3, N, 2, N * N, L), F32)],
            in_specs=[any_] * 3,
            out_specs=[any_, vmem],
            scratch_shapes=[pltpu.VMEM((N, N, T, w), BF16) for w in widths]
            + [pltpu.VMEM((3, N, N, 8, L), F32), pltpu.VMEM((3, N, 2, N * N, L), F32)]
            + [pltpu.VMEM((N, N, 2 * N, C, w), BF16) for w in widths] + [pltpu.VMEM((N, 2, N, C, w), BF16) for w in widths]
            + [dma((3,)), dma((3, 3)), dma((3, 4)), dma((3, 4)), dma((3, 4, N)), dma((3, 4, N)), dma((3,)), dma((3,)), dma((3, 4)), dma((3, 4)),
               dma((3,)), dma((3,)), dma((3,)), dma((3, N, 2)), dma((3,))],
            compiler_params=params,
        )(x, rows, meta)
        out = pl.pallas_call(
            functools.partial(_experts, cols),
            name='experts',
            out_shape=[jax.ShapeDtypeStruct((T, D), BF16)] + [jax.ShapeDtypeStruct((N, K * C, w), BF16) for w in widths]
            + [jax.ShapeDtypeStruct((N, len(LATER), C, w), BF16) for w in widths],
            in_specs=[any_] * 4 + [vmem],
            out_specs=[vmem] + [any_] * 6,
            scratch_shapes=[
                pltpu.VMEM((D, ff), BF16), pltpu.VMEM((D, ff), BF16), pltpu.VMEM((ff, D), BF16),
                pltpu.VMEM((2, 2, N, 2, C, D), BF16), pltpu.VMEM((2 * L, ff), BF16), pltpu.VMEM((N, N, N, 2, C, D), BF16),
                *(pltpu.VMEM((N, len(ONCE), C, w), BF16) for w in widths),
                *(pltpu.VMEM((N, T, w), F32) for w in widths), *(pltpu.VMEM((2, T, w), F32) for w in widths),
                *(pltpu.VMEM((2, T // 2, w), F32) for w in widths),
                dma((3,)), dma((2, 2)), dma((3,)), dma((3,)), dma((3,)), dma((3,)), dma((3,)), dma((3, len(ONCE))), dma((3, len(LATER))), dma((3,)),
                dma((N,)), dma((3, 4)), dma((3, 4)),
            ],
            compiler_params=params,
        )(xin, w1, w3, w2, metas)
        return out[0]

    return jax.shard_map(local, mesh=mesh, in_specs=(tok, P(None, None), tok, wsp, wsp, wsp), out_specs=tok, check_vma=False)
```

```python
import functools

import jax
import jax.numpy as jnp
from jax import lax
from jax.experimental import pallas as pl
from jax.experimental.pallas import tpu as pltpu
from jax.sharding import PartitionSpec as P

MESH = pl.DeviceIdType.MESH
F32 = jnp.float32
BF16 = jnp.bfloat16
N = 4


def _cols(d):
    t = d // 128
    w = [(t // 3) * 128, (t // 3) * 128, (t - 2 * (t // 3)) * 128]
    return [(0, w[0]), (w[0], w[1]), (w[0] + w[1], w[2])]


def _where():
    o, e = lax.axis_index('outer'), lax.axis_index('expert')
    return o // N, o % N, e // 2, e % 2


def _dev(z, y, x, c):
    return (0, z * N + y, x * 2 + c)


def _along(p, me, a):
    z, y, x, c = me
    return _dev(*((a, y, x, c), (z, a, x, c), (z, y, a, c))[p])


def _plane(p, me, b, d, c):
    z, y, x, _ = me
    return _dev(*((z, b, d, c), (b, y, d, c), (b, d, x, c))[p])


def _copy(src, dst, send, recv, dev):
    return pltpu.make_async_remote_copy(src_ref=src, dst_ref=dst, send_sem=send, recv_sem=recv, device_id=dev, device_id_type=MESH)


def _wait(ref, sem):
    pltpu.make_async_copy(ref, ref, sem).wait()


def _hops(o):
    return o - 2 * (o // 3)


def _step(o, s):
    return (o + N - s * (o // 2) * (1 - o // 3)) % N


def _order(p, a, b, d):
    return ((a, b, d), (d, a, b), (b, d, a))[p]


def _dispatch(cols, x_ref, rows_ref, meta_ref, xin, meta_out, ag0, ag1, ag2, mt, mb, sb0, sb1, sb2, rl0, rl1, rl2,
              own, lown, asend, arecv, bsend, brecv, tsend, trecv, msend, mrecv, lsend, send, fsend, rrecv, recv):
    me = _where()
    z, y, x, c = me
    ag, sb, rl = (ag0, ag1, ag2), (sb0, sb1, sb2), (rl0, rl1, rl2)
    T = x_ref.shape[0]
    C = sb0.shape[3]
    L = 2 * N * C
    h = T // 2
    axis = (z, y, x)
    base = ((z, y, x), (y, x, z), (x, z, y))
    which = (0, 0, 1)
    parts = range(3)
    sides = (1, 3)
    halves = (pl.ds(0, h), pl.ds(h, h))

    def to_a(p, k):
        a, b, d = base[p]
        return _dev(*_order(p, (a + k) % N, b, d), c)

    def to_b(p, k):
        a, b, d = base[p]
        return _dev(*_order(p, a, (b + k) % N, d), c)

    def give_b(p, k, src):
        a, b, d = base[p]
        for q in range(2):
            _copy(src, ag[p].at[(a + k) % N, b], bsend.at[p, q, k], brecv.at[p, q, k], to_b(p, sides[q])).start()

    def pass_b(p, k):
        a, b, d = base[p]
        for q in range(2):
            _wait(ag[p].at[0, 0], brecv.at[p, q, k])
            blk = ag[p].at[(a + k) % N, (b + (3, 1)[q]) % N, halves[q]]
            _copy(blk, blk, bsend.at[p, 2 + q, k], brecv.at[p, 2 + q, k], to_b(p, sides[q])).start()

    for p in parts:
        a, b, d = base[p]
        blk = x_ref.at[:, pl.ds(*cols[p])]
        for q in range(2):
            _copy(blk, ag[p].at[a, b], asend.at[p, q], arecv.at[p, q], to_a(p, sides[q])).start()
        pltpu.make_async_copy(blk, ag[p].at[a, b], lown.at[p, 0]).start()
    for p in parts:
        a, b, d = base[p]
        for ka in range(N):
            for kb in range(N):
                at = _dev(*_order(p, (a + ka) % N, (b + kb) % N, d), c)
                src = rows_ref.at[p, (a + ka) % N * N + (b + kb) % N]
                if ka + kb:
                    _copy(src, mt.at[p, a, b], tsend.at[p], trecv.at[p], at).start()
                else:
                    pltpu.make_async_copy(src, mt.at[p, a, b], lown.at[p, 1]).start()
    for p in parts:
        give_b(p, 0, x_ref.at[:, pl.ds(*cols[p])])
    for p in parts:
        a, b, d = base[p]
        for q in range(2):
            _wait(ag[p].at[0, 0], arecv.at[p, q])
            blk = ag[p].at[(a + (3, 1)[q]) % N, b, halves[q]]
            _copy(blk, blk, asend.at[p, 2 + q], arecv.at[p, 2 + q], to_a(p, sides[q])).start()
    for p in parts:
        a, b, d = base[p]
        for k in sides:
            give_b(p, k, ag[p].at[(a + k) % N, b])
    for p in parts:
        for k in (1, 3, 2):
            _copy(meta_ref.at[which[p]], mb.at[p, axis[p]], msend.at[p, k], mrecv.at[p, k], _along(p, me, (axis[p] + k) % N)).start()
        pltpu.make_async_copy(meta_ref.at[which[p]], mb.at[p, axis[p]], lown.at[p, 2]).start()
    for p in parts:
        pass_b(p, 0)
    for p in parts:
        a, b, d = base[p]
        for q in range(2):
            _wait(ag[p].at[0, 0, halves[q]], arecv.at[p, 2 + q])
        give_b(p, 2, ag[p].at[(a + 2) % N, b])
        _wait(ag[p].at[0, 0], lown.at[p, 0])
        _wait(mt.at[p, 0, 0], lown.at[p, 1])
        _wait(rows_ref.at[p, pl.ds(0, N * N - 1)], trecv.at[p])

    def final(p, bs, ds):
        i = _order(p, slice(None), bs, ds)
        return xin.at[i[0], i[1], i[2], c, :, pl.ds(*cols[p])]

    def select(p, bo):
        a_, b, d = base[p]
        w = cols[p][1]
        bs = (b + bo) % N

        @pl.loop(0, N)
        def _(a):
            hot = lax.broadcasted_iota(jnp.int32, (T, L), 0).astype(F32) == mt[p, a, bs, 0:1, :]
            hot = jnp.where(hot, 1.0, 0.0).astype(BF16)
            r = lax.dot_general(hot, ag[p][a, bs], (((0,), (0,)), ((), ())), preferred_element_type=F32)
            sb[p][a, bo] = r.astype(BF16).reshape(2 * N, C, w)

        for do in (2, 1, 3, 0):
            for cc in range(2):
                s = 1 - 2 * cc
                src = sb[p].at[:, bo, (d + do) % N * 2 + (c + cc) % 2]
                if do == 2:
                    to = _dev(*_order(p, a_, b, (d + N + s) % N), c)
                    _copy(src, rl[p].at[bo, cc], lsend.at[p], rrecv.at[p, bo, cc], to).start()
                elif do + cc:
                    to = _dev(*_order(p, a_, b, (d + do) % N), (c + cc) % 2)
                    _copy(src, final(p, bs, d), send.at[p], recv.at[p], to).start()
                else:
                    pltpu.make_async_copy(src, final(p, bs, d), own.at[p]).start()

    def relay(p, bo):
        a, b, d = base[p]
        for cc in range(2):
            s = 1 - 2 * cc
            _wait(rl[p].at[bo, cc], rrecv.at[p, bo, cc])
            to = _dev(*_order(p, a, b, (d + N + s) % N), (c + cc) % 2)
            _copy(rl[p].at[bo, cc], final(p, (b + bo) % N, (d + N - s) % N), fsend.at[p], recv.at[p], to).start()

    for p in parts:
        select(p, 0)
    for p in parts:
        for k in sides:
            pass_b(p, k)
    for p in parts:
        relay(p, 0)
        pass_b(p, 2)
    for p in parts:
        for bo in sides:
            select(p, bo)
    for p in parts:
        for k in range(N):
            for q in range(2):
                _wait(ag[p].at[0, 0, halves[q]], brecv.at[p, 2 + q, k])
        select(p, 2)
    for p in parts:
        for bo in sides:
            relay(p, bo)
    for p in parts:
        relay(p, 2)
    for p in parts:
        _wait(mb.at[p, 0], lown.at[p, 2])
        for k in (1, 2, 3):
            _wait(mb.at[p, 0], mrecv.at[p, k])
    meta_out[...] = mb[...]
    for p in parts:
        for k in (1, 2, 3):
            _wait(mb.at[p, 0], msend.at[p, k])
        _wait(rows_ref.at[p, pl.ds(0, N * N - 1)], tsend.at[p])
        for q in range(2):
            _wait(ag[p].at[0, 0], asend.at[p, q])
            _wait(ag[p].at[0, 0, halves[q]], asend.at[p, 2 + q])
            for k in range(N):
                _wait(ag[p].at[0, 0], bsend.at[p, q, k])
                _wait(ag[p].at[0, 0, halves[q]], bsend.at[p, 2 + q, k])
        _wait(sb[p].at[:, :, 0], own.at[p])
        _wait(sb[p].at[:, :, pl.ds(0, 2)], fsend.at[p])
        _wait(sb[p].at[:, :, pl.ds(0, 2)], lsend.at[p])
        _wait(sb[p].at[:, :, pl.ds(0, 5)], send.at[p])
        _wait(sb[p].at[:, :, pl.ds(0, 7)], recv.at[p])


FIRST_B = (False, True, False)


def _bd(p, f, g):
    return (f, g) if FIRST_B[p] else (g, f)


def _spot(fo, go, cc, r):
    sf, sg = (1 - 2 * ((o + cc) % 2) for o in (go, fo))
    nf = max(r - _hops(go), 0) if cc else min(r, _hops(fo))
    ng = r - nf
    return (N + {0: 0, 1: 1, 2: sf, 3: -1}[fo] * nf) % N, (N + {0: 0, 1: 1, 2: sg, 3: -1}[go] * ng) % N


WAYS = [(fo, go, cc) for fo in (2, 1, 3, 0) for go in (2, 1, 3, 0) for cc in range(2)]
LATER = [(k, r) for r in (2, 3) for k in WAYS if _hops(k[0]) + _hops(k[1]) > r]
ONCE = [k for k in WAYS if _hops(k[0]) + _hops(k[1]) > 1]
NEAR = 2 * N * N - len(ONCE) - 1

TILES = [((2, 1), (2, 3)), ((1, 2), (3, 2)), ((2, 2), (2, 0)), ((1, 1), (3, 3)),
         ((1, 3), (3, 1)), ((0, 2), (0, 0)), ((1, 0), (3, 0)), ((0, 1), (0, 3))]


def _ready(p, fo, go):
    return max(st for st, t in enumerate(TILES) for zo, yo in t if ((yo == go), (zo == fo), (zo, yo) == (go, fo))[p])


def _later(parts, r):
    n = {k: _hops(k[0]) + _hops(k[1]) for k in ONCE}
    return sorted(((p, k, r) for k in ONCE for p in parts if n[k] > r), key=lambda v: (_ready(v[0], *v[1][:2]), -n[v[1]], -v[0]))


def _pick(values, s):
    return sum(v * (1 - ((s - k) * (s - k) + 63) // 64) for k, v in enumerate(values))


def _experts(cols, xin, w1_ref, w3_ref, w2_ref, meta, y_ref, r0, r1, r2, rm0, rm1, rm2, w1, w3, w2, xb, hb, ob, rl0, rl1, rl2,
             s0, s1, s2, q0, q1, q2, h0, h1, h2,
             wsem, xsem, own, lsend, send, fsend, isend, rrecv, irecv, recv, bsem, ssend, srecv):
    me = _where()
    z, y, x, c = me
    R, rl, rm = (r0, r1, r2), (rl0, rl1, rl2), (rm0, rm1, rm2)
    C, D = xin.shape[4:]
    G = 2 * N * C
    ff = w1.shape[1]
    steps = len(TILES)
    base = ((y, x), (z, x), (z, y))
    axis = (z, y, x)
    loads = [pltpu.make_async_copy(s.at[0], d, wsem.at[q]) for q, (s, d) in enumerate(((w1_ref, w1), (w3_ref, w3), (w2_ref, w2)))]

    def cell(st, q):
        zo, yo = TILES[st][q]
        return (z + zo) % N, (y + yo) % N

    def load(st):
        for q in range(2):
            zt, yv = cell(st, q)
            pltpu.make_async_copy(xin.at[zt, yv], xb.at[st % 2, q], xsem.at[st % 2, q]).start()

    load(0)
    for q in loads:
        q.start()
    cs = [pl.ds(lo, w) for lo, w in cols]

    def at(p, f, g, cc):
        bo, do = _bd(p, f, g)
        return _plane(p, me, (base[p][0] + bo) % N, (base[p][1] + do) % N, (c + cc) % 2)

    def slot(p, b, d):
        return R[p].at[:, pl.ds(((b * N + d) * 2 + c) * C, C)]

    def put(p, fo, go, cc, lead, src):
        bo, do = _bd(p, fo, go)
        b, d, c2 = (base[p][0] + bo) % N, (base[p][1] + do) % N, (c + cc) % 2
        dst = R[p].at[lead, pl.ds(((base[p][0] * N + base[p][1]) * 2 + c) * C, C)]
        n = _hops(fo) + _hops(go)
        if n > 1:
            k = ONCE.index((fo, go, cc))
            _copy(src, rl[p].at[lead, k], lsend.at[p], rrecv.at[p, k], at(p, *_spot(fo, go, cc, 1), 0)).start()
        elif n + cc:
            _copy(src, dst, send.at[p], recv.at[p], _plane(p, me, b, d, c2)).start()
        else:
            pltpu.make_async_copy(src, dst, own.at[p]).start()

    def give(st):
        for cc in range(2):
            c2 = (c + cc) % 2
            for q in range(2):
                zo, yo = TILES[st][q]
                zt, yv = cell(st, q)
                put(2, yo, zo, cc, slice(None), ob.at[zt, yv, :, c2, :, cs[2]])
        for do in (2, 1, 3, 0):
            x2 = (x + do) % N
            for cc in range(2):
                c2 = (c + cc) % 2
                for q in range(2):
                    zo, yo = TILES[st][q]
                    zt, yv = cell(st, q)
                    put(0, do, yo, cc, zt, ob.at[zt, yv, x2, c2, :, cs[0]])
                    put(1, zo, do, cc, yv, ob.at[zt, yv, x2, c2, :, cs[1]])

    def forward(p, key, r):
        fo, go, cc = key
        here, there = _spot(fo, go, cc, r), _spot(fo, go, cc, r + 1)
        if r == 1:
            k = ONCE.index(key)
            buf, sem = rl[p].at[:, k], rrecv.at[p, k]
        else:
            k = LATER.index((key, r))
            buf, sem = rm[p].at[:, k], irecv.at[p, k]
        _wait(buf, sem)
        hop = [(there[q] + N - here[q]) % N for q in range(2)]
        if r + 1 == _hops(fo) + _hops(go):
            bs, ds = ((base[p][q] + N - v) % N for q, v in enumerate(_bd(p, *here)))
            _copy(buf, slot(p, bs, ds), fsend.at[p], recv.at[p], at(p, *hop, cc)).start()
        else:
            k = LATER.index((key, r + 1))
            _copy(buf, rm[p].at[:, k], isend.at[p], irecv.at[p, k], at(p, *hop, 0)).start()

    fs, ds = min(256, ff), min(512, D)

    @pl.loop(0, steps)
    def _(s):
        zt = [(z + _pick([t[q][0] for t in TILES], s)) % N for q in range(2)]
        yt = [(y + _pick([t[q][1] for t in TILES], s)) % N for q in range(2)]
        for st in range(steps - 1):
            @pl.when(s == st)
            def _():
                load(st + 1)

        for q in range(2):
            _wait(xb.at[0, q], xsem.at[s % 2, q])

        @pl.when(s == 0)
        def _():
            for q in loads[:2]:
                q.wait()

        @pl.loop(0, ff // fs)
        def _(f):
            fc = pl.ds(pl.multiple_of(f * fs, fs), fs)
            xt = xb[s % 2].reshape(2 * G, D)
            a = jnp.dot(xt, w1[:, fc], preferred_element_type=F32)
            b = jnp.dot(xt, w3[:, fc], preferred_element_type=F32)
            hb[:, fc] = (jax.nn.silu(a) * b).astype(BF16)

        @pl.when(s == 0)
        def _():
            loads[2].wait()

        @pl.loop(0, D // ds)
        def _(f):
            fc = pl.ds(pl.multiple_of(f * ds, ds), ds)
            o = jnp.dot(hb[...], w2[:, fc], preferred_element_type=F32).astype(BF16)
            ob[zt[0], yt[0], :, :, :, fc] = o[:G].reshape(N, 2, C, ds)
            ob[zt[1], yt[1], :, :, :, fc] = o[G:].reshape(N, 2, C, ds)

        for st in range(steps):
            @pl.when(s == st)
            def _():
                give(st)

    S, Q, H = (s0, s1, s2), (q0, q1, q2), (h0, h1, h2)
    T = y_ref.shape[0]
    L = 2 * N * C
    h = T // 2
    halves = (pl.ds(0, h), pl.ds(h, h))
    sides = (1, 3)

    def room(k, p):
        return (w1, w3)[k // 2].at[pl.ds(k % 2 * N * L, N * L), pl.ds(0, cols[p][1])]

    def gather(p):
        _wait(slot(p, 0, 0), own.at[p])
        _wait(R[p].at[:, pl.ds(0, (2 * N * N - 1) * C)], recv.at[p])
        for k in (2, 1, 3, 0):
            pltpu.make_async_copy(R[p].at[(axis[p] + k) % N], room(k, p), bsem.at[k]).start()

    def partial(p, k):
        a = (axis[p] + k) % N
        _wait(room(k, p), bsem.at[k])

        @pl.loop(0, N)
        def _(b):
            row = (z * N + b, b * N + y, b * N + x)[p]
            tab = meta[p, a, 0, pl.ds(row, 1), :]
            g = meta[p, a, 1, pl.ds(row, 1), :]
            hot = lax.broadcasted_iota(jnp.int32, (T, L), 0).astype(F32) == tab
            m = jnp.where(hot, g, 0.0)
            here = pl.ds(pl.multiple_of(b * L, L), L)
            for q in range(3):
                part = m.astype(BF16)
                w2[q * T:(q + 1) * T, here] = part
                m = m - part.astype(F32)

        t = jnp.dot(w2[:, pl.ds(0, N * L)], room(k, p)[...], preferred_element_type=F32)
        S[p][k] = t[:T] + t[T:2 * T] + t[2 * T:]

    def side(p, q):
        return _along(p, me, (axis[p] + sides[q]) % N)

    def halfway(p):
        for q in range(2):
            _copy(S[p].at[2, halves[q]], H[p].at[q], ssend.at[p, q], srecv.at[p, q], side(p, q)).start()

    def hand(p, q, e, at_):
        _copy(S[p].at[sides[q], halves[e]], Q[p].at[q, halves[e]], ssend.at[p, at_ + q], srecv.at[p, at_ + q], side(p, q)).start()

    def onwards(*args):
        for v in _later(*args):
            forward(*v)

    onwards((2, 1, 0), 1)
    onwards((2,), 2)
    onwards((2,), 3)
    onwards((1, 0), 2)
    for p in (2, 1, 0):
        gather(p)
        partial(p, 2)
        halfway(p)
        if p == 2:
            onwards((1, 0), 3)
        for q in range(2):
            partial(p, sides[q])
            hand(p, q, 1 - q, 2)
        for q in range(2):
            _wait(H[p].at[q], srecv.at[p, q])
            S[p][sides[q], halves[q]] += H[p][q]
            hand(p, q, q, 4)
        partial(p, 0)
    for p in (2, 1, 0):
        t = S[p][0]
        for q in range(2):
            for e in (2, 4):
                _wait(H[p].at[q], srecv.at[p, e + q])
            t += Q[p][q]
        y_ref[:, cs[p]] = t.astype(BF16)
    for p in range(3):
        for q in range(2):
            for e in (0, 2, 4):
                _wait(H[p].at[q], ssend.at[p, e + q])
        _wait(R[p].at[:, pl.ds(0, NEAR * C)], send.at[p])
        _wait(R[p].at[:, pl.ds(0, len(ONCE) * C)], lsend.at[p])
        _wait(R[p].at[:, pl.ds(0, len(ONCE) * C)], fsend.at[p])
        _wait(R[p].at[:, pl.ds(0, len(LATER) * C)], isend.at[p])


def _plan(x, wr, idx, cap):
    T = x.shape[0]
    E = wr.shape[1]
    logits = jnp.dot(x, wr, preferred_element_type=F32)
    oh = idx[:, :, None] == jnp.arange(E, dtype=idx.dtype)
    g = jax.nn.softmax(jnp.sum(jnp.where(oh, logits[:, None, :], 0.0), axis=-1), axis=-1)
    m = jnp.sum(oh, axis=1, dtype=jnp.int32).astype(F32)
    ge = jnp.sum(jnp.where(oh, g[:, :, None], 0.0), axis=1)
    pos = jnp.arange(T, dtype=jnp.int32)
    tri = (pos[None, :] < pos[:, None]).astype(BF16)
    cnt = jnp.dot(tri, m.astype(BF16), preferred_element_type=F32)
    cnt = jnp.where(m > 0, cnt, -1.0)
    hit = cnt[:, :, None] == jnp.arange(cap, dtype=F32)
    tab = jnp.sum(jnp.where(hit, pos.astype(F32)[:, None, None] + 1.0, 0.0), axis=0) - 1.0
    gw = jnp.sum(jnp.where(hit, ge[:, :, None], 0.0), axis=0)

    def both(v):
        v = v.reshape(N, N, N, 2 * cap)
        return v.reshape(N * N, 2 * N * cap), v.transpose(0, 2, 1, 3).reshape(N * N, 2 * N * cap)

    (t0, t2), (g0, g2) = both(tab), both(gw)
    t = tab.reshape(N, N, N, 2 * cap)
    rows = jnp.stack([t, t.transpose(1, 2, 0, 3), t.transpose(2, 0, 1, 3)]).reshape(3, N * N, 1, 2 * N * cap)
    return jnp.broadcast_to(rows, (3, N * N, 8, 2 * N * cap)), jnp.stack([jnp.stack([t0, g0]), jnp.stack([t2, g2])])


def solution(mesh):
    assert (mesh.shape['outer'], mesh.shape['expert']) == (N * N, 2 * N)
    tok = P(('data', 'outer', 'expert'), None)
    wsp = P(('outer', 'expert'), None, None)
    any_ = pl.BlockSpec(memory_space=pl.ANY)
    vmem = pl.BlockSpec(memory_space=pltpu.VMEM)
    dma = pltpu.SemaphoreType.DMA
    params = pltpu.CompilerParams(has_side_effects=True, vmem_limit_bytes=67043328)

    def local(x, wr, idx, w1, w3, w2):
        T, D = x.shape
        E = wr.shape[1]
        C = 2 * T * idx.shape[1] // E
        ff = w1.shape[2]
        cols = _cols(D)
        widths = [w for _, w in cols]
        L = 2 * N * C
        K = 2 * N * N
        rows, meta = _plan(x, wr, idx, C)
        xin, metas = pl.pallas_call(
            functools.partial(_dispatch, cols),
            name='dispatch',
            out_shape=[jax.ShapeDtypeStruct((N, N, N, 2, C, D), BF16), jax.ShapeDtypeStruct((3, N, 2, N * N, L), F32)],
            in_specs=[any_] * 3,
            out_specs=[any_, vmem],
            scratch_shapes=[pltpu.VMEM((N, N, T, w), BF16) for w in widths]
            + [pltpu.VMEM((3, N, N, 8, L), F32), pltpu.VMEM((3, N, 2, N * N, L), F32)]
            + [pltpu.VMEM((N, N, 2 * N, C, w), BF16) for w in widths] + [pltpu.VMEM((N, 2, N, C, w), BF16) for w in widths]
            + [dma((3,)), dma((3, 3)), dma((3, 4)), dma((3, 4)), dma((3, 4, N)), dma((3, 4, N)), dma((3,)), dma((3,)), dma((3, 4)), dma((3, 4)),
               dma((3,)), dma((3,)), dma((3,)), dma((3, N, 2)), dma((3,))],
            compiler_params=params,
        )(x, rows, meta)
        out = pl.pallas_call(
            functools.partial(_experts, cols),
            name='experts',
            out_shape=[jax.ShapeDtypeStruct((T, D), BF16)] + [jax.ShapeDtypeStruct((N, K * C, w), BF16) for w in widths]
            + [jax.ShapeDtypeStruct((N, len(LATER), C, w), BF16) for w in widths],
            in_specs=[any_] * 4 + [vmem],
            out_specs=[vmem] + [any_] * 6,
            scratch_shapes=[
                pltpu.VMEM((D, ff), BF16), pltpu.VMEM((D, ff), BF16), pltpu.VMEM((ff, D), BF16),
                pltpu.VMEM((2, 2, N, 2, C, D), BF16), pltpu.VMEM((2 * L, ff), BF16), pltpu.VMEM((N, N, N, 2, C, D), BF16),
                *(pltpu.VMEM((N, len(ONCE), C, w), BF16) for w in widths),
                *(pltpu.VMEM((N, T, w), F32) for w in widths), *(pltpu.VMEM((2, T, w), F32) for w in widths),
                *(pltpu.VMEM((2, T // 2, w), F32) for w in widths),
                dma((3,)), dma((2, 2)), dma((3,)), dma((3,)), dma((3,)), dma((3,)), dma((3,)), dma((3, len(ONCE))), dma((3, len(LATER))), dma((3,)),
                dma((N,)), dma((3, 6)), dma((3, 6)),
            ],
            compiler_params=params,
        )(xin, w1, w3, w2, metas)
        return out[0]

    return jax.shard_map(local, mesh=mesh, in_specs=(tok, P(None, None), tok, wsp, wsp, wsp), out_specs=tok, check_vma=False)
```

```python
import functools

import jax
import jax.numpy as jnp
from jax import lax
from jax.experimental import pallas as pl
from jax.experimental.pallas import tpu as pltpu
from jax.sharding import PartitionSpec as P

MESH = pl.DeviceIdType.MESH
F32 = jnp.float32
BF16 = jnp.bfloat16
N = 4


def _cols(d):
    t = d // 128
    w = [(t // 3) * 128, (t // 3) * 128, (t - 2 * (t // 3)) * 128]
    return [(0, w[0]), (w[0], w[1]), (w[0] + w[1], w[2])]


def _where():
    o, e = lax.axis_index('outer'), lax.axis_index('expert')
    return o // N, o % N, e // 2, e % 2


def _dev(z, y, x, c):
    return (0, z * N + y, x * 2 + c)


def _along(p, me, a):
    z, y, x, c = me
    return _dev(*((a, y, x, c), (z, a, x, c), (z, y, a, c))[p])


def _plane(p, me, b, d, c):
    z, y, x, _ = me
    return _dev(*((z, b, d, c), (b, y, d, c), (b, d, x, c))[p])


def _copy(src, dst, send, recv, dev):
    return pltpu.make_async_remote_copy(src_ref=src, dst_ref=dst, send_sem=send, recv_sem=recv, device_id=dev, device_id_type=MESH)


def _wait(ref, sem):
    pltpu.make_async_copy(ref, ref, sem).wait()


def _hops(o):
    return o - 2 * (o // 3)


def _step(o, s):
    return (o + N - s * (o // 2) * (1 - o // 3)) % N


def _order(p, a, b, d):
    return ((a, b, d), (d, a, b), (b, d, a))[p]


def _dispatch(cols, x_ref, rows_ref, meta_ref, xin, meta_out, ag0, ag1, ag2, mt, mb, sb0, sb1, sb2, rl0, rl1, rl2,
              own, lown, asend, arecv, bsend, brecv, tsend, trecv, msend, mrecv, lsend, send, fsend, rrecv, recv):
    me = _where()
    z, y, x, c = me
    ag, sb, rl = (ag0, ag1, ag2), (sb0, sb1, sb2), (rl0, rl1, rl2)
    T = x_ref.shape[0]
    C = sb0.shape[3]
    L = 2 * N * C
    h = T // 2
    axis = (z, y, x)
    base = ((z, y, x), (y, x, z), (x, z, y))
    which = (0, 0, 1)
    parts = range(3)
    sides = (1, 3)
    halves = (pl.ds(0, h), pl.ds(h, h))

    def to_a(p, k):
        a, b, d = base[p]
        return _dev(*_order(p, (a + k) % N, b, d), c)

    def to_b(p, k):
        a, b, d = base[p]
        return _dev(*_order(p, a, (b + k) % N, d), c)

    def give_b(p, k, src):
        a, b, d = base[p]
        for q in range(2):
            _copy(src, ag[p].at[(a + k) % N, b], bsend.at[p, q, k], brecv.at[p, q, k], to_b(p, sides[q])).start()

    def pass_b(p, k):
        a, b, d = base[p]
        for q in range(2):
            _wait(ag[p].at[0, 0], brecv.at[p, q, k])
            blk = ag[p].at[(a + k) % N, (b + (3, 1)[q]) % N, halves[q]]
            _copy(blk, blk, bsend.at[p, 2 + q, k], brecv.at[p, 2 + q, k], to_b(p, sides[q])).start()

    for p in parts:
        a, b, d = base[p]
        blk = x_ref.at[:, pl.ds(*cols[p])]
        for q in range(2):
            _copy(blk, ag[p].at[a, b], asend.at[p, q], arecv.at[p, q], to_a(p, sides[q])).start()
        pltpu.make_async_copy(blk, ag[p].at[a, b], lown.at[p, 0]).start()
    for p in parts:
        a, b, d = base[p]
        for ka in range(N):
            for kb in range(N):
                at = _dev(*_order(p, (a + ka) % N, (b + kb) % N, d), c)
                src = rows_ref.at[p, (a + ka) % N * N + (b + kb) % N]
                if ka + kb:
                    _copy(src, mt.at[p, a, b], tsend.at[p], trecv.at[p], at).start()
                else:
                    pltpu.make_async_copy(src, mt.at[p, a, b], lown.at[p, 1]).start()
    for p in parts:
        give_b(p, 0, x_ref.at[:, pl.ds(*cols[p])])
    for p in parts:
        a, b, d = base[p]
        for q in range(2):
            _wait(ag[p].at[0, 0], arecv.at[p, q])
            blk = ag[p].at[(a + (3, 1)[q]) % N, b, halves[q]]
            _copy(blk, blk, asend.at[p, 2 + q], arecv.at[p, 2 + q], to_a(p, sides[q])).start()
    for p in parts:
        a, b, d = base[p]
        for k in sides:
            give_b(p, k, ag[p].at[(a + k) % N, b])
    for p in parts:
        for k in (1, 3, 2):
            _copy(meta_ref.at[which[p]], mb.at[p, axis[p]], msend.at[p, k], mrecv.at[p, k], _along(p, me, (axis[p] + k) % N)).start()
        pltpu.make_async_copy(meta_ref.at[which[p]], mb.at[p, axis[p]], lown.at[p, 2]).start()
    for p in parts:
        pass_b(p, 0)
    for p in parts:
        a, b, d = base[p]
        for q in range(2):
            _wait(ag[p].at[0, 0, halves[q]], arecv.at[p, 2 + q])
        give_b(p, 2, ag[p].at[(a + 2) % N, b])
        _wait(ag[p].at[0, 0], lown.at[p, 0])
        _wait(mt.at[p, 0, 0], lown.at[p, 1])
        _wait(rows_ref.at[p, pl.ds(0, N * N - 1)], trecv.at[p])

    def final(p, bs, ds):
        i = _order(p, slice(None), bs, ds)
        return xin.at[i[0], i[1], i[2], c, :, pl.ds(*cols[p])]

    def select(p, bo):
        a_, b, d = base[p]
        w = cols[p][1]
        bs = (b + bo) % N

        @pl.loop(0, N)
        def _(a):
            hot = lax.broadcasted_iota(jnp.int32, (T, L), 0).astype(F32) == mt[p, a, bs, 0:1, :]
            hot = jnp.where(hot, 1.0, 0.0).astype(BF16)
            r = lax.dot_general(hot, ag[p][a, bs], (((0,), (0,)), ((), ())), preferred_element_type=F32)
            sb[p][a, bo] = r.astype(BF16).reshape(2 * N, C, w)

        for do in (2, 1, 3, 0):
            for cc in range(2):
                s = 1 - 2 * cc
                src = sb[p].at[:, bo, (d + do) % N * 2 + (c + cc) % 2]
                if do == 2:
                    to = _dev(*_order(p, a_, b, (d + N + s) % N), c)
                    _copy(src, rl[p].at[bo, cc], lsend.at[p], rrecv.at[p, bo, cc], to).start()
                elif do + cc:
                    to = _dev(*_order(p, a_, b, (d + do) % N), (c + cc) % 2)
                    _copy(src, final(p, bs, d), send.at[p], recv.at[p], to).start()
                else:
                    pltpu.make_async_copy(src, final(p, bs, d), own.at[p]).start()

    def relay(p, bo):
        a, b, d = base[p]
        for cc in range(2):
            s = 1 - 2 * cc
            _wait(rl[p].at[bo, cc], rrecv.at[p, bo, cc])
            to = _dev(*_order(p, a, b, (d + N + s) % N), (c + cc) % 2)
            _copy(rl[p].at[bo, cc], final(p, (b + bo) % N, (d + N - s) % N), fsend.at[p], recv.at[p], to).start()

    for p in parts:
        select(p, 0)
    for p in parts:
        for k in sides:
            pass_b(p, k)
    for p in parts:
        relay(p, 0)
        pass_b(p, 2)
    for p in parts:
        for bo in sides:
            select(p, bo)
    for p in parts:
        for k in range(N):
            for q in range(2):
                _wait(ag[p].at[0, 0, halves[q]], brecv.at[p, 2 + q, k])
        select(p, 2)
    for p in parts:
        for bo in sides:
            relay(p, bo)
    for p in parts:
        relay(p, 2)
    for p in parts:
        _wait(mb.at[p, 0], lown.at[p, 2])
        for k in (1, 2, 3):
            _wait(mb.at[p, 0], mrecv.at[p, k])
    meta_out[...] = mb[...]
    for p in parts:
        for k in (1, 2, 3):
            _wait(mb.at[p, 0], msend.at[p, k])
        _wait(rows_ref.at[p, pl.ds(0, N * N - 1)], tsend.at[p])
        for q in range(2):
            _wait(ag[p].at[0, 0], asend.at[p, q])
            _wait(ag[p].at[0, 0, halves[q]], asend.at[p, 2 + q])
            for k in range(N):
                _wait(ag[p].at[0, 0], bsend.at[p, q, k])
                _wait(ag[p].at[0, 0, halves[q]], bsend.at[p, 2 + q, k])
        _wait(sb[p].at[:, :, 0], own.at[p])
        _wait(sb[p].at[:, :, pl.ds(0, 2)], fsend.at[p])
        _wait(sb[p].at[:, :, pl.ds(0, 2)], lsend.at[p])
        _wait(sb[p].at[:, :, pl.ds(0, 5)], send.at[p])
        _wait(sb[p].at[:, :, pl.ds(0, 7)], recv.at[p])


FIRST_B = (False, True, False)


def _bd(p, f, g):
    return (f, g) if FIRST_B[p] else (g, f)


def _spot(fo, go, cc, r):
    sf, sg = (1 - 2 * ((o + cc) % 2) for o in (go, fo))
    nf = max(r - _hops(go), 0) if cc else min(r, _hops(fo))
    ng = r - nf
    return (N + {0: 0, 1: 1, 2: sf, 3: -1}[fo] * nf) % N, (N + {0: 0, 1: 1, 2: sg, 3: -1}[go] * ng) % N


WAYS = [(fo, go, cc) for fo in (2, 1, 3, 0) for go in (2, 1, 3, 0) for cc in range(2)]
LATER = [(k, r) for r in (2, 3) for k in WAYS if _hops(k[0]) + _hops(k[1]) > r]
ONCE = [k for k in WAYS if _hops(k[0]) + _hops(k[1]) > 1]
NEAR = 2 * N * N - len(ONCE) - 1

TILES = [((2, 2), (0, 2)), ((1, 2), (3, 2)), ((2, 1), (2, 3)), ((2, 0), (0, 0)),
         ((1, 1), (3, 3)), ((1, 3), (3, 1)), ((1, 0), (3, 0)), ((0, 1), (0, 3))]
LAG = 3


def _ready(p, fo, go):
    return max(st for st, t in enumerate(TILES) for zo, yo in t if ((yo == go), (zo == fo), (zo, yo) == (go, fo))[p])


def _when(p, key, r):
    n, st = _hops(key[0]) + _hops(key[1]), _ready(p, *key[:2]) + LAG * r
    return st if n > 2 and st < len(TILES) else len(TILES)


def _later(parts, r, at=len(TILES)):
    n = {k: _hops(k[0]) + _hops(k[1]) for k in ONCE}
    return sorted(((p, k, r) for k in ONCE for p in parts if n[k] > r and _when(p, k, r) == at),
                  key=lambda v: (_ready(v[0], *v[1][:2]), -n[v[1]], -v[0]))


def _pick(values, s):
    return sum(v * (1 - ((s - k) * (s - k) + 63) // 64) for k, v in enumerate(values))


def _experts(cols, xin, w1_ref, w3_ref, w2_ref, meta, y_ref, r0, r1, r2, rm0, rm1, rm2, w1, w3, w2, xb, hb, ob, rl0, rl1, rl2,
             s0, s1, s2, q0, q1, q2, h0, h1, h2,
             wsem, xsem, own, lsend, send, fsend, isend, rrecv, irecv, recv, bsem, ssend, srecv):
    me = _where()
    z, y, x, c = me
    R, rl, rm = (r0, r1, r2), (rl0, rl1, rl2), (rm0, rm1, rm2)
    C, D = xin.shape[4:]
    G = 2 * N * C
    ff = w1.shape[1]
    steps = len(TILES)
    base = ((y, x), (z, x), (z, y))
    axis = (z, y, x)
    loads = [pltpu.make_async_copy(s.at[0], d, wsem.at[q]) for q, (s, d) in enumerate(((w1_ref, w1), (w3_ref, w3), (w2_ref, w2)))]

    def cell(st, q):
        zo, yo = TILES[st][q]
        return (z + zo) % N, (y + yo) % N

    def load(st):
        for q in range(2):
            zt, yv = cell(st, q)
            pltpu.make_async_copy(xin.at[zt, yv], xb.at[st % 2, q], xsem.at[st % 2, q]).start()

    load(0)
    for q in loads:
        q.start()
    cs = [pl.ds(lo, w) for lo, w in cols]

    def at(p, f, g, cc):
        bo, do = _bd(p, f, g)
        return _plane(p, me, (base[p][0] + bo) % N, (base[p][1] + do) % N, (c + cc) % 2)

    def slot(p, b, d):
        return R[p].at[:, pl.ds(((b * N + d) * 2 + c) * C, C)]

    def put(p, fo, go, cc, lead, src):
        bo, do = _bd(p, fo, go)
        b, d, c2 = (base[p][0] + bo) % N, (base[p][1] + do) % N, (c + cc) % 2
        dst = R[p].at[lead, pl.ds(((base[p][0] * N + base[p][1]) * 2 + c) * C, C)]
        n = _hops(fo) + _hops(go)
        if n > 1:
            k = ONCE.index((fo, go, cc))
            _copy(src, rl[p].at[lead, k], lsend.at[p], rrecv.at[p, k], at(p, *_spot(fo, go, cc, 1), 0)).start()
        elif n + cc:
            _copy(src, dst, send.at[p], recv.at[p], _plane(p, me, b, d, c2)).start()
        else:
            pltpu.make_async_copy(src, dst, own.at[p]).start()

    def give(st):
        for cc in range(2):
            c2 = (c + cc) % 2
            for q in range(2):
                zo, yo = TILES[st][q]
                zt, yv = cell(st, q)
                put(2, yo, zo, cc, slice(None), ob.at[zt, yv, :, c2, :, cs[2]])
        for do in (2, 1, 3, 0):
            x2 = (x + do) % N
            for cc in range(2):
                c2 = (c + cc) % 2
                for q in range(2):
                    zo, yo = TILES[st][q]
                    zt, yv = cell(st, q)
                    put(0, do, yo, cc, zt, ob.at[zt, yv, x2, c2, :, cs[0]])
                    put(1, zo, do, cc, yv, ob.at[zt, yv, x2, c2, :, cs[1]])

    def forward(p, key, r):
        fo, go, cc = key
        here, there = _spot(fo, go, cc, r), _spot(fo, go, cc, r + 1)
        if r == 1:
            k = ONCE.index(key)
            buf, sem = rl[p].at[:, k], rrecv.at[p, k]
        else:
            k = LATER.index((key, r))
            buf, sem = rm[p].at[:, k], irecv.at[p, k]
        _wait(buf, sem)
        hop = [(there[q] + N - here[q]) % N for q in range(2)]
        if r + 1 == _hops(fo) + _hops(go):
            bs, ds = ((base[p][q] + N - v) % N for q, v in enumerate(_bd(p, *here)))
            _copy(buf, slot(p, bs, ds), fsend.at[p], recv.at[p], at(p, *hop, cc)).start()
        else:
            k = LATER.index((key, r + 1))
            _copy(buf, rm[p].at[:, k], isend.at[p], irecv.at[p, k], at(p, *hop, 0)).start()

    fs, ds = min(256, ff), min(512, D)

    @pl.loop(0, steps)
    def _(s):
        zt = [(z + _pick([t[q][0] for t in TILES], s)) % N for q in range(2)]
        yt = [(y + _pick([t[q][1] for t in TILES], s)) % N for q in range(2)]
        for st in range(steps - 1):
            @pl.when(s == st)
            def _():
                load(st + 1)

        for q in range(2):
            _wait(xb.at[0, q], xsem.at[s % 2, q])

        @pl.when(s == 0)
        def _():
            for q in loads[:2]:
                q.wait()

        @pl.loop(0, ff // fs)
        def _(f):
            fc = pl.ds(pl.multiple_of(f * fs, fs), fs)
            xt = xb[s % 2].reshape(2 * G, D)
            a = jnp.dot(xt, w1[:, fc], preferred_element_type=F32)
            b = jnp.dot(xt, w3[:, fc], preferred_element_type=F32)
            hb[:, fc] = (jax.nn.silu(a) * b).astype(BF16)

        @pl.when(s == 0)
        def _():
            loads[2].wait()

        @pl.loop(0, D // ds)
        def _(f):
            fc = pl.ds(pl.multiple_of(f * ds, ds), ds)
            o = jnp.dot(hb[...], w2[:, fc], preferred_element_type=F32).astype(BF16)
            ob[zt[0], yt[0], :, :, :, fc] = o[:G].reshape(N, 2, C, ds)
            ob[zt[1], yt[1], :, :, :, fc] = o[G:].reshape(N, 2, C, ds)

        for st in range(steps):
            @pl.when(s == st)
            def _():
                give(st)
                for r in (1, 2, 3):
                    for v in _later((2, 1, 0), r, st):
                        forward(*v)

    S, Q, H = (s0, s1, s2), (q0, q1, q2), (h0, h1, h2)
    T = y_ref.shape[0]
    L = 2 * N * C
    h = T // 2
    halves = (pl.ds(0, h), pl.ds(h, h))
    sides = (1, 3)

    def room(k, p):
        return (w1, w3)[k // 2].at[pl.ds(k % 2 * N * L, N * L), pl.ds(0, cols[p][1])]

    def gather(p):
        _wait(slot(p, 0, 0), own.at[p])
        _wait(R[p].at[:, pl.ds(0, (2 * N * N - 1) * C)], recv.at[p])
        for k in (2, 1, 3, 0):
            pltpu.make_async_copy(R[p].at[(axis[p] + k) % N], room(k, p), bsem.at[k]).start()

    def partial(p, k):
        a = (axis[p] + k) % N
        _wait(room(k, p), bsem.at[k])

        @pl.loop(0, N)
        def _(b):
            row = (z * N + b, b * N + y, b * N + x)[p]
            tab = meta[p, a, 0, pl.ds(row, 1), :]
            g = meta[p, a, 1, pl.ds(row, 1), :]
            hot = lax.broadcasted_iota(jnp.int32, (T, L), 0).astype(F32) == tab
            m = jnp.where(hot, g, 0.0)
            here = pl.ds(pl.multiple_of(b * L, L), L)
            for q in range(3):
                part = m.astype(BF16)
                w2[q * T:(q + 1) * T, here] = part
                m = m - part.astype(F32)

        t = jnp.dot(w2[:, pl.ds(0, N * L)], room(k, p)[...], preferred_element_type=F32)
        S[p][k] = t[:T] + t[T:2 * T] + t[2 * T:]

    def side(p, q):
        return _along(p, me, (axis[p] + sides[q]) % N)

    def halfway(p):
        for q in range(2):
            _copy(S[p].at[2, halves[q]], H[p].at[q], ssend.at[p, q], srecv.at[p, q], side(p, q)).start()

    def hand(p, q, e, at_):
        _copy(S[p].at[sides[q], halves[e]], Q[p].at[q, halves[e]], ssend.at[p, at_ + q], srecv.at[p, at_ + q], side(p, q)).start()

    def onwards(*args):
        for v in _later(*args):
            forward(*v)

    onwards((2, 1, 0), 1)
    onwards((2,), 2)
    onwards((2,), 3)
    onwards((1, 0), 2)
    for p in (2, 1, 0):
        gather(p)
        partial(p, 2)
        halfway(p)
        if p == 2:
            onwards((1, 0), 3)
        for q in range(2):
            partial(p, sides[q])
            hand(p, q, 1 - q, 2)
        for q in range(2):
            _wait(H[p].at[q], srecv.at[p, q])
            S[p][sides[q], halves[q]] += H[p][q]
            hand(p, q, q, 4)
        partial(p, 0)
    for p in (2, 1, 0):
        t = S[p][0]
        for q in range(2):
            for e in (2, 4):
                _wait(H[p].at[q], srecv.at[p, e + q])
            t += Q[p][q]
        y_ref[:, cs[p]] = t.astype(BF16)
    for p in range(3):
        for q in range(2):
            for e in (0, 2, 4):
                _wait(H[p].at[q], ssend.at[p, e + q])
        _wait(R[p].at[:, pl.ds(0, NEAR * C)], send.at[p])
        _wait(R[p].at[:, pl.ds(0, len(ONCE) * C)], lsend.at[p])
        _wait(R[p].at[:, pl.ds(0, len(ONCE) * C)], fsend.at[p])
        _wait(R[p].at[:, pl.ds(0, len(LATER) * C)], isend.at[p])


def _plan(x, wr, idx, cap):
    T = x.shape[0]
    E = wr.shape[1]
    logits = jnp.dot(x, wr, preferred_element_type=F32)
    oh = idx[:, :, None] == jnp.arange(E, dtype=idx.dtype)
    g = jax.nn.softmax(jnp.sum(jnp.where(oh, logits[:, None, :], 0.0), axis=-1), axis=-1)
    m = jnp.sum(oh, axis=1, dtype=jnp.int32).astype(F32)
    ge = jnp.sum(jnp.where(oh, g[:, :, None], 0.0), axis=1)
    pos = jnp.arange(T, dtype=jnp.int32)
    tri = (pos[None, :] < pos[:, None]).astype(BF16)
    cnt = jnp.dot(tri, m.astype(BF16), preferred_element_type=F32)
    cnt = jnp.where(m > 0, cnt, -1.0)
    hit = cnt[:, :, None] == jnp.arange(cap, dtype=F32)
    tab = jnp.sum(jnp.where(hit, pos.astype(F32)[:, None, None] + 1.0, 0.0), axis=0) - 1.0
    gw = jnp.sum(jnp.where(hit, ge[:, :, None], 0.0), axis=0)

    def both(v):
        v = v.reshape(N, N, N, 2 * cap)
        return v.reshape(N * N, 2 * N * cap), v.transpose(0, 2, 1, 3).reshape(N * N, 2 * N * cap)

    (t0, t2), (g0, g2) = both(tab), both(gw)
    t = tab.reshape(N, N, N, 2 * cap)
    rows = jnp.stack([t, t.transpose(1, 2, 0, 3), t.transpose(2, 0, 1, 3)]).reshape(3, N * N, 1, 2 * N * cap)
    return jnp.broadcast_to(rows, (3, N * N, 8, 2 * N * cap)), jnp.stack([jnp.stack([t0, g0]), jnp.stack([t2, g2])])


def solution(mesh):
    assert (mesh.shape['outer'], mesh.shape['expert']) == (N * N, 2 * N)
    tok = P(('data', 'outer', 'expert'), None)
    wsp = P(('outer', 'expert'), None, None)
    any_ = pl.BlockSpec(memory_space=pl.ANY)
    vmem = pl.BlockSpec(memory_space=pltpu.VMEM)
    dma = pltpu.SemaphoreType.DMA
    params = pltpu.CompilerParams(has_side_effects=True, vmem_limit_bytes=67043328)

    def local(x, wr, idx, w1, w3, w2):
        T, D = x.shape
        E = wr.shape[1]
        C = 2 * T * idx.shape[1] // E
        ff = w1.shape[2]
        cols = _cols(D)
        widths = [w for _, w in cols]
        L = 2 * N * C
        K = 2 * N * N
        rows, meta = _plan(x, wr, idx, C)
        xin, metas = pl.pallas_call(
            functools.partial(_dispatch, cols),
            name='dispatch',
            out_shape=[jax.ShapeDtypeStruct((N, N, N, 2, C, D), BF16), jax.ShapeDtypeStruct((3, N, 2, N * N, L), F32)],
            in_specs=[any_] * 3,
            out_specs=[any_, vmem],
            scratch_shapes=[pltpu.VMEM((N, N, T, w), BF16) for w in widths]
            + [pltpu.VMEM((3, N, N, 8, L), F32), pltpu.VMEM((3, N, 2, N * N, L), F32)]
            + [pltpu.VMEM((N, N, 2 * N, C, w), BF16) for w in widths] + [pltpu.VMEM((N, 2, N, C, w), BF16) for w in widths]
            + [dma((3,)), dma((3, 3)), dma((3, 4)), dma((3, 4)), dma((3, 4, N)), dma((3, 4, N)), dma((3,)), dma((3,)), dma((3, 4)), dma((3, 4)),
               dma((3,)), dma((3,)), dma((3,)), dma((3, N, 2)), dma((3,))],
            compiler_params=params,
        )(x, rows, meta)
        out = pl.pallas_call(
            functools.partial(_experts, cols),
            name='experts',
            out_shape=[jax.ShapeDtypeStruct((T, D), BF16)] + [jax.ShapeDtypeStruct((N, K * C, w), BF16) for w in widths]
            + [jax.ShapeDtypeStruct((N, len(LATER), C, w), BF16) for w in widths],
            in_specs=[any_] * 4 + [vmem],
            out_specs=[vmem] + [any_] * 6,
            scratch_shapes=[
                pltpu.VMEM((D, ff), BF16), pltpu.VMEM((D, ff), BF16), pltpu.VMEM((ff, D), BF16),
                pltpu.VMEM((2, 2, N, 2, C, D), BF16), pltpu.VMEM((2 * L, ff), BF16), pltpu.VMEM((N, N, N, 2, C, D), BF16),
                *(pltpu.VMEM((N, len(ONCE), C, w), BF16) for w in widths),
                *(pltpu.VMEM((N, T, w), F32) for w in widths), *(pltpu.VMEM((2, T, w), F32) for w in widths),
                *(pltpu.VMEM((2, T // 2, w), F32) for w in widths),
                dma((3,)), dma((2, 2)), dma((3,)), dma((3,)), dma((3,)), dma((3,)), dma((3,)), dma((3, len(ONCE))), dma((3, len(LATER))), dma((3,)),
                dma((N,)), dma((3, 6)), dma((3, 6)),
            ],
            compiler_params=params,
        )(xin, w1, w3, w2, metas)
        return out[0]

    return jax.shard_map(local, mesh=mesh, in_specs=(tok, P(None, None), tok, wsp, wsp, wsp), out_specs=tok, check_vma=False)
```

```python
import functools

import jax
import jax.numpy as jnp
from jax import lax
from jax.experimental import pallas as pl
from jax.experimental.pallas import tpu as pltpu
from jax.sharding import PartitionSpec as P

MESH = pl.DeviceIdType.MESH
F32 = jnp.float32
BF16 = jnp.bfloat16
N = 4
PAIR, PARTS = range(2), range(3)
FAR_FIRST = (2, 1, 3, 0)


def _cols(d):
    t = d // 128
    w = [(t // 3) * 128, (t // 3) * 128, (t - 2 * (t // 3)) * 128]
    return [(0, w[0]), (w[0], w[1]), (w[0] + w[1], w[2])]


def _where():
    o, e = lax.axis_index('outer'), lax.axis_index('expert')
    return o // N, o % N, e // 2, e % 2


def _dev(z, y, x, c):
    return (0, z * N + y, x * 2 + c)


def _along(p, me, a):
    z, y, x, c = me
    return _dev(*((a, y, x, c), (z, a, x, c), (z, y, a, c))[p])


def _plane(p, me, b, d, c):
    z, y, x, _ = me
    return _dev(*((z, b, d, c), (b, y, d, c), (b, d, x, c))[p])


def _copy(src, dst, send, recv, dev):
    return pltpu.make_async_remote_copy(src_ref=src, dst_ref=dst, send_sem=send, recv_sem=recv, device_id=dev, device_id_type=MESH)


def _wait(ref, sem):
    pltpu.make_async_copy(ref, ref, sem).wait()


def _hops(o):
    return o - 2 * (o // 3)


def _step(o, s):
    return (o + N - s * (o // 2) * (1 - o // 3)) % N


def _order(p, a, b, d):
    return ((a, b, d), (d, a, b), (b, d, a))[p]


def _dispatch(cols, x_ref, rows_ref, meta_ref, xin, meta_out, ag0, ag1, ag2, mt, mb, sb0, sb1, sb2, rl0, rl1, rl2,
              own, lown, asend, arecv, bsend, brecv, tsend, trecv, msend, mrecv, lsend, send, fsend, rrecv, recv):
    me = _where()
    z, y, x, c = me
    ag, sb, rl = (ag0, ag1, ag2), (sb0, sb1, sb2), (rl0, rl1, rl2)
    T = x_ref.shape[0]
    C = sb0.shape[3]
    L = 2 * N * C
    h = T // 2
    axis = (z, y, x)
    base = ((z, y, x), (y, x, z), (x, z, y))
    which = (0, 0, 1)
    parts = PARTS
    sides = (1, 3)
    halves = (pl.ds(0, h), pl.ds(h, h))

    def to_a(p, k):
        a, b, d = base[p]
        return _dev(*_order(p, (a + k) % N, b, d), c)

    def to_b(p, k):
        a, b, d = base[p]
        return _dev(*_order(p, a, (b + k) % N, d), c)

    def give_b(p, k, src):
        a, b, d = base[p]
        for q in PAIR:
            _copy(src, ag[p].at[(a + k) % N, b], bsend.at[p, q, k], brecv.at[p, q, k], to_b(p, sides[q])).start()

    def pass_b(p, k):
        a, b, d = base[p]
        for q in PAIR:
            _wait(ag[p].at[0, 0], brecv.at[p, q, k])
            blk = ag[p].at[(a + k) % N, (b + (3, 1)[q]) % N, halves[q]]
            _copy(blk, blk, bsend.at[p, 2 + q, k], brecv.at[p, 2 + q, k], to_b(p, sides[q])).start()

    for p in parts:
        a, b, d = base[p]
        blk = x_ref.at[:, pl.ds(*cols[p])]
        for q in PAIR:
            _copy(blk, ag[p].at[a, b], asend.at[p, q], arecv.at[p, q], to_a(p, sides[q])).start()
        pltpu.make_async_copy(blk, ag[p].at[a, b], lown.at[p, 0]).start()
    for p in parts:
        a, b, d = base[p]
        for ka in range(N):
            for kb in range(N):
                at = _dev(*_order(p, (a + ka) % N, (b + kb) % N, d), c)
                src = rows_ref.at[p, (a + ka) % N * N + (b + kb) % N]
                if ka + kb:
                    _copy(src, mt.at[p, a, b], tsend.at[p], trecv.at[p], at).start()
                else:
                    pltpu.make_async_copy(src, mt.at[p, a, b], lown.at[p, 1]).start()
    for p in parts:
        give_b(p, 0, x_ref.at[:, pl.ds(*cols[p])])
    for p in parts:
        a, b, d = base[p]
        for q in PAIR:
            _wait(ag[p].at[0, 0], arecv.at[p, q])
            blk = ag[p].at[(a + (3, 1)[q]) % N, b, halves[q]]
            _copy(blk, blk, asend.at[p, 2 + q], arecv.at[p, 2 + q], to_a(p, sides[q])).start()
    for p in parts:
        a, b, d = base[p]
        for k in sides:
            give_b(p, k, ag[p].at[(a + k) % N, b])
    for p in parts:
        for k in (1, 3, 2):
            _copy(meta_ref.at[which[p]], mb.at[p, axis[p]], msend.at[p, k], mrecv.at[p, k], _along(p, me, (axis[p] + k) % N)).start()
        pltpu.make_async_copy(meta_ref.at[which[p]], mb.at[p, axis[p]], lown.at[p, 2]).start()
    for p in parts:
        pass_b(p, 0)
    for p in parts:
        a, b, d = base[p]
        for q in PAIR:
            _wait(ag[p].at[0, 0, halves[q]], arecv.at[p, 2 + q])
        give_b(p, 2, ag[p].at[(a + 2) % N, b])
        _wait(ag[p].at[0, 0], lown.at[p, 0])
        _wait(mt.at[p, 0, 0], lown.at[p, 1])
        _wait(rows_ref.at[p, pl.ds(0, N * N - 1)], trecv.at[p])

    def final(p, bs, ds):
        i = _order(p, slice(None), bs, ds)
        return xin.at[i[0], i[1], i[2], c, :, pl.ds(*cols[p])]

    def select(p, bo):
        a_, b, d = base[p]
        w = cols[p][1]
        bs = (b + bo) % N

        @pl.loop(0, N)
        def _(a):
            hot = lax.broadcasted_iota(jnp.int32, (T, L), 0).astype(F32) == mt[p, a, bs, 0:1, :]
            hot = jnp.where(hot, 1.0, 0.0).astype(BF16)
            r = lax.dot_general(hot, ag[p][a, bs], (((0,), (0,)), ((), ())), preferred_element_type=F32)
            sb[p][a, bo] = r.astype(BF16).reshape(2 * N, C, w)

        for do in FAR_FIRST:
            for cc in PAIR:
                s = 1 - 2 * cc
                src = sb[p].at[:, bo, (d + do) % N * 2 + (c + cc) % 2]
                if do == 2:
                    to = _dev(*_order(p, a_, b, (d + N + s) % N), c)
                    _copy(src, rl[p].at[bo, cc], lsend.at[p], rrecv.at[p, bo, cc], to).start()
                elif do + cc:
                    to = _dev(*_order(p, a_, b, (d + do) % N), (c + cc) % 2)
                    _copy(src, final(p, bs, d), send.at[p], recv.at[p], to).start()
                else:
                    pltpu.make_async_copy(src, final(p, bs, d), own.at[p]).start()

    def relay(p, bo):
        a, b, d = base[p]
        for cc in PAIR:
            s = 1 - 2 * cc
            _wait(rl[p].at[bo, cc], rrecv.at[p, bo, cc])
            to = _dev(*_order(p, a, b, (d + N + s) % N), (c + cc) % 2)
            _copy(rl[p].at[bo, cc], final(p, (b + bo) % N, (d + N - s) % N), fsend.at[p], recv.at[p], to).start()

    for p in parts:
        select(p, 0)
    for p in parts:
        for k in sides:
            pass_b(p, k)
    for p in parts:
        relay(p, 0)
        pass_b(p, 2)
    for p in parts:
        for bo in sides:
            select(p, bo)
    for p in parts:
        for k in range(N):
            for q in PAIR:
                _wait(ag[p].at[0, 0, halves[q]], brecv.at[p, 2 + q, k])
        select(p, 2)
    for p in parts:
        for bo in sides:
            relay(p, bo)
    for p in parts:
        relay(p, 2)
    for p in parts:
        _wait(mb.at[p, 0], lown.at[p, 2])
        for k in (1, 2, 3):
            _wait(mb.at[p, 0], mrecv.at[p, k])
    meta_out[...] = mb[...]
    for p in parts:
        for k in (1, 2, 3):
            _wait(mb.at[p, 0], msend.at[p, k])
        _wait(rows_ref.at[p, pl.ds(0, N * N - 1)], tsend.at[p])
        for q in PAIR:
            _wait(ag[p].at[0, 0], asend.at[p, q])
            _wait(ag[p].at[0, 0, halves[q]], asend.at[p, 2 + q])
            for k in range(N):
                _wait(ag[p].at[0, 0], bsend.at[p, q, k])
                _wait(ag[p].at[0, 0, halves[q]], bsend.at[p, 2 + q, k])
        _wait(sb[p].at[:, :, 0], own.at[p])
        _wait(sb[p].at[:, :, pl.ds(0, 2)], fsend.at[p])
        _wait(sb[p].at[:, :, pl.ds(0, 2)], lsend.at[p])
        _wait(sb[p].at[:, :, pl.ds(0, 5)], send.at[p])
        _wait(sb[p].at[:, :, pl.ds(0, 7)], recv.at[p])


FIRST_B = (False, True, False)


def _bd(p, f, g):
    return (f, g) if FIRST_B[p] else (g, f)


def _spot(fo, go, cc, r):
    sf, sg = (1 - 2 * ((o + cc) % 2) for o in (go, fo))
    nf = max(r - _hops(go), 0) if cc else min(r, _hops(fo))
    ng = r - nf
    return (N + {0: 0, 1: 1, 2: sf, 3: -1}[fo] * nf) % N, (N + {0: 0, 1: 1, 2: sg, 3: -1}[go] * ng) % N


WAYS = [(fo, go, cc) for fo in FAR_FIRST for go in FAR_FIRST for cc in PAIR]
LATER = [(k, r) for r in (2, 3) for k in WAYS if _hops(k[0]) + _hops(k[1]) > r]
ONCE = [k for k in WAYS if _hops(k[0]) + _hops(k[1]) > 1]
NEAR = 2 * N * N - len(ONCE) - 1

TILES = [((2, 1), (2, 3)), ((1, 2), (3, 2)), ((2, 2), (2, 0)), ((1, 1), (3, 3)),
         ((1, 3), (3, 1)), ((0, 2), (0, 0)), ((1, 0), (3, 0)), ((0, 1), (0, 3))]


def _ready(p, fo, go):
    return max(st for st, t in enumerate(TILES) for zo, yo in t if ((yo == go), (zo == fo), (zo, yo) == (go, fo))[p])


def _later(parts, r):
    n = {k: _hops(k[0]) + _hops(k[1]) for k in ONCE}
    return sorted(((p, k, r) for k in ONCE for p in parts if n[k] > r), key=lambda v: (_ready(v[0], *v[1][:2]), -n[v[1]], -v[0]))


def _pick(values, s):
    return sum(v * (1 - ((s - k) * (s - k) + 63) // 64) for k, v in enumerate(values))


def _experts(cols, xin, w1_ref, w3_ref, w2_ref, meta, y_ref, r0, r1, r2, rm0, rm1, rm2, w1, w3, w2, xb, hb, ob, rl0, rl1, rl2,
             s0, s1, s2, q0, q1, q2, h0, h1, h2,
             wsem, xsem, own, lsend, send, fsend, isend, rrecv, irecv, recv, bsem, ssend, srecv):
    me = _where()
    z, y, x, c = me
    R, rl, rm = (r0, r1, r2), (rl0, rl1, rl2), (rm0, rm1, rm2)
    C, D = xin.shape[4:]
    G = 2 * N * C
    ff = w1.shape[1]
    steps = len(TILES)
    base = ((y, x), (z, x), (z, y))
    axis = (z, y, x)
    loads = [pltpu.make_async_copy(s.at[0], d, wsem.at[q]) for q, (s, d) in enumerate(((w1_ref, w1), (w3_ref, w3), (w2_ref, w2)))]

    def cell(st, q):
        zo, yo = TILES[st][q]
        return (z + zo) % N, (y + yo) % N

    def load(st):
        for q in PAIR:
            zt, yv = cell(st, q)
            pltpu.make_async_copy(xin.at[zt, yv], xb.at[st % 2, q], xsem.at[st % 2, q]).start()

    load(0)
    for q in loads:
        q.start()
    cs = [pl.ds(lo, w) for lo, w in cols]

    def at(p, f, g, cc):
        bo, do = _bd(p, f, g)
        return _plane(p, me, (base[p][0] + bo) % N, (base[p][1] + do) % N, (c + cc) % 2)

    def slot(p, b, d):
        return R[p].at[:, pl.ds(((b * N + d) * 2 + c) * C, C)]

    def put(p, fo, go, cc, lead, src):
        bo, do = _bd(p, fo, go)
        b, d, c2 = (base[p][0] + bo) % N, (base[p][1] + do) % N, (c + cc) % 2
        dst = R[p].at[lead, pl.ds(((base[p][0] * N + base[p][1]) * 2 + c) * C, C)]
        n = _hops(fo) + _hops(go)
        if n > 1:
            k = ONCE.index((fo, go, cc))
            _copy(src, rl[p].at[lead, k], lsend.at[p], rrecv.at[p, k], at(p, *_spot(fo, go, cc, 1), 0)).start()
        elif n + cc:
            _copy(src, dst, send.at[p], recv.at[p], _plane(p, me, b, d, c2)).start()
        else:
            pltpu.make_async_copy(src, dst, own.at[p]).start()

    def give(st):
        for cc in PAIR:
            c2 = (c + cc) % 2
            for q in PAIR:
                zo, yo = TILES[st][q]
                zt, yv = cell(st, q)
                put(2, yo, zo, cc, slice(None), ob.at[zt, yv, :, c2, :, cs[2]])
        for do in FAR_FIRST:
            x2 = (x + do) % N
            for cc in PAIR:
                c2 = (c + cc) % 2
                for q in PAIR:
                    zo, yo = TILES[st][q]
                    zt, yv = cell(st, q)
                    put(0, do, yo, cc, zt, ob.at[zt, yv, x2, c2, :, cs[0]])
                    put(1, zo, do, cc, yv, ob.at[zt, yv, x2, c2, :, cs[1]])

    def forward(p, key, r):
        fo, go, cc = key
        here, there = _spot(fo, go, cc, r), _spot(fo, go, cc, r + 1)
        if r == 1:
            k = ONCE.index(key)
            buf, sem = rl[p].at[:, k], rrecv.at[p, k]
        else:
            k = LATER.index((key, r))
            buf, sem = rm[p].at[:, k], irecv.at[p, k]
        _wait(buf, sem)
        hop = [(there[q] + N - here[q]) % N for q in PAIR]
        if r + 1 == _hops(fo) + _hops(go):
            bs, ds = ((base[p][q] + N - v) % N for q, v in enumerate(_bd(p, *here)))
            _copy(buf, slot(p, bs, ds), fsend.at[p], recv.at[p], at(p, *hop, cc)).start()
        else:
            k = LATER.index((key, r + 1))
            _copy(buf, rm[p].at[:, k], isend.at[p], irecv.at[p, k], at(p, *hop, 0)).start()

    fs, ds = min(256, ff), min(512, D)

    @pl.loop(0, steps)
    def _(s):
        zt = [(z + _pick([t[q][0] for t in TILES], s)) % N for q in PAIR]
        yt = [(y + _pick([t[q][1] for t in TILES], s)) % N for q in PAIR]
        for st in range(steps - 1):
            @pl.when(s == st)
            def _():
                load(st + 1)

        for q in PAIR:
            _wait(xb.at[0, q], xsem.at[s % 2, q])

        @pl.when(s == 0)
        def _():
            for q in loads[:2]:
                q.wait()

        @pl.loop(0, ff // fs)
        def _(f):
            fc = pl.ds(pl.multiple_of(f * fs, fs), fs)
            xt = xb[s % 2].reshape(2 * G, D)
            a = jnp.dot(xt, w1[:, fc], preferred_element_type=F32)
            b = jnp.dot(xt, w3[:, fc], preferred_element_type=F32)
            hb[:, fc] = (jax.nn.silu(a) * b).astype(BF16)

        @pl.when(s == 0)
        def _():
            loads[2].wait()

        @pl.loop(0, D // ds)
        def _(f):
            fc = pl.ds(pl.multiple_of(f * ds, ds), ds)
            o = jnp.dot(hb[...], w2[:, fc], preferred_element_type=F32).astype(BF16)
            ob[zt[0], yt[0], :, :, :, fc] = o[:G].reshape(N, 2, C, ds)
            ob[zt[1], yt[1], :, :, :, fc] = o[G:].reshape(N, 2, C, ds)

        for st in range(steps):
            @pl.when(s == st)
            def _():
                give(st)

    S, Q, H = (s0, s1, s2), (q0, q1, q2), (h0, h1, h2)
    T = y_ref.shape[0]
    L = 2 * N * C
    h = T // 2
    halves = (pl.ds(0, h), pl.ds(h, h))
    sides = (1, 3)

    def room(k, p):
        return (w1, w3)[k // 2].at[pl.ds(k % 2 * N * L, N * L), pl.ds(0, cols[p][1])]

    def arrived(p):
        _wait(slot(p, 0, 0), own.at[p])
        _wait(R[p].at[:, pl.ds(0, (2 * N * N - 1) * C)], recv.at[p])

    def fetch(p, *ks):
        for k in ks:
            pltpu.make_async_copy(R[p].at[(axis[p] + k) % N], room(k, p), bsem.at[k]).start()

    def partial(p, k):
        a = (axis[p] + k) % N
        _wait(room(k, p), bsem.at[k])

        @pl.loop(0, N)
        def _(b):
            row = (z * N + b, b * N + y, b * N + x)[p]
            tab = meta[p, a, 0, pl.ds(row, 1), :]
            g = meta[p, a, 1, pl.ds(row, 1), :]
            hot = lax.broadcasted_iota(jnp.int32, (T, L), 0).astype(F32) == tab
            m = jnp.where(hot, g, 0.0)
            here = pl.ds(pl.multiple_of(b * L, L), L)
            for q in PARTS:
                part = m.astype(BF16)
                w2[q * T:(q + 1) * T, here] = part
                m = m - part.astype(F32)

        t = jnp.dot(w2[:, pl.ds(0, N * L)], room(k, p)[...], preferred_element_type=F32)
        S[p][k] = t[:T] + t[T:2 * T] + t[2 * T:]

    def side(p, q):
        return _along(p, me, (axis[p] + sides[q]) % N)

    def halfway(p):
        for q in PAIR:
            _copy(S[p].at[2, halves[q]], H[p].at[q], ssend.at[p, q], srecv.at[p, q], side(p, q)).start()

    def hand(p, q, e, at_):
        _copy(S[p].at[sides[q], halves[e]], Q[p].at[q, halves[e]], ssend.at[p, at_ + q], srecv.at[p, at_ + q], side(p, q)).start()

    def onwards(*args):
        for v in _later(*args):
            forward(*v)

    onwards((2, 1, 0), 1)
    onwards((2,), 2)
    onwards((2,), 3)
    onwards((1, 0), 2)
    def outward(p):
        for q in PAIR:
            partial(p, sides[q])
            hand(p, q, 1 - q, 2)

    def finish(p):
        for q in PAIR:
            _wait(H[p].at[q], srecv.at[p, q])
            S[p][sides[q], halves[q]] += H[p][q]
            hand(p, q, q, 4)

    arrived(2)
    fetch(2, *FAR_FIRST)
    partial(2, 2)
    halfway(2)
    onwards((1, 0), 3)
    outward(2)
    partial(2, 0)
    finish(2)
    arrived(1)
    fetch(1, *FAR_FIRST)
    partial(1, 2)
    halfway(1)
    outward(1)
    arrived(0)
    fetch(0, 2, 1, 3)
    partial(0, 2)
    halfway(0)
    outward(0)
    finish(1)
    partial(1, 0)
    fetch(0, 0)
    finish(0)
    partial(0, 0)
    for p in (2, 1, 0):
        t = S[p][0]
        for q in PAIR:
            for e in (2, 4):
                _wait(H[p].at[q], srecv.at[p, e + q])
            t += Q[p][q]
        y_ref[:, cs[p]] = t.astype(BF16)
    for p in PARTS:
        for q in PAIR:
            for e in (0, 2, 4):
                _wait(H[p].at[q], ssend.at[p, e + q])
        _wait(R[p].at[:, pl.ds(0, NEAR * C)], send.at[p])
        _wait(R[p].at[:, pl.ds(0, len(ONCE) * C)], lsend.at[p])
        _wait(R[p].at[:, pl.ds(0, len(ONCE) * C)], fsend.at[p])
        _wait(R[p].at[:, pl.ds(0, len(LATER) * C)], isend.at[p])


def _plan(x, wr, idx, cap):
    T = x.shape[0]
    E = wr.shape[1]
    logits = jnp.dot(x, wr, preferred_element_type=F32)
    oh = idx[:, :, None] == jnp.arange(E, dtype=idx.dtype)
    g = jax.nn.softmax(jnp.sum(jnp.where(oh, logits[:, None, :], 0.0), axis=-1), axis=-1)
    m = jnp.sum(oh, axis=1, dtype=jnp.int32).astype(F32)
    ge = jnp.sum(jnp.where(oh, g[:, :, None], 0.0), axis=1)
    pos = jnp.arange(T, dtype=jnp.int32)
    tri = (pos[None, :] < pos[:, None]).astype(BF16)
    cnt = jnp.dot(tri, m.astype(BF16), preferred_element_type=F32)
    cnt = jnp.where(m > 0, cnt, -1.0)
    hit = cnt[:, :, None] == jnp.arange(cap, dtype=F32)
    tab = jnp.sum(jnp.where(hit, pos.astype(F32)[:, None, None] + 1.0, 0.0), axis=0) - 1.0
    gw = jnp.sum(jnp.where(hit, ge[:, :, None], 0.0), axis=0)

    def both(v):
        v = v.reshape(N, N, N, 2 * cap)
        return v.reshape(N * N, 2 * N * cap), v.transpose(0, 2, 1, 3).reshape(N * N, 2 * N * cap)

    (t0, t2), (g0, g2) = both(tab), both(gw)
    t = tab.reshape(N, N, N, 2 * cap)
    rows = jnp.stack([t, t.transpose(1, 2, 0, 3), t.transpose(2, 0, 1, 3)]).reshape(3, N * N, 1, 2 * N * cap)
    return jnp.broadcast_to(rows, (3, N * N, 8, 2 * N * cap)), jnp.stack([jnp.stack([t0, g0]), jnp.stack([t2, g2])])


def solution(mesh):
    assert (mesh.shape['outer'], mesh.shape['expert']) == (N * N, 2 * N)
    tok = P(('data', 'outer', 'expert'), None)
    wsp = P(('outer', 'expert'), None, None)
    any_ = pl.BlockSpec(memory_space=pl.ANY)
    vmem = pl.BlockSpec(memory_space=pltpu.VMEM)
    dma = pltpu.SemaphoreType.DMA
    params = pltpu.CompilerParams(has_side_effects=True, vmem_limit_bytes=67043328)

    def local(x, wr, idx, w1, w3, w2):
        T, D = x.shape
        E = wr.shape[1]
        C = 2 * T * idx.shape[1] // E
        ff = w1.shape[2]
        cols = _cols(D)
        widths = [w for _, w in cols]
        L = 2 * N * C
        K = 2 * N * N
        rows, meta = _plan(x, wr, idx, C)
        xin, metas = pl.pallas_call(
            functools.partial(_dispatch, cols),
            name='dispatch',
            out_shape=[jax.ShapeDtypeStruct((N, N, N, 2, C, D), BF16), jax.ShapeDtypeStruct((3, N, 2, N * N, L), F32)],
            in_specs=[any_] * 3,
            out_specs=[any_, vmem],
            scratch_shapes=[pltpu.VMEM((N, N, T, w), BF16) for w in widths]
            + [pltpu.VMEM((3, N, N, 8, L), F32), pltpu.VMEM((3, N, 2, N * N, L), F32)]
            + [pltpu.VMEM((N, N, 2 * N, C, w), BF16) for w in widths] + [pltpu.VMEM((N, 2, N, C, w), BF16) for w in widths]
            + [dma((3,)), dma((3, 3)), dma((3, 4)), dma((3, 4)), dma((3, 4, N)), dma((3, 4, N)), dma((3,)), dma((3,)), dma((3, 4)), dma((3, 4)),
               dma((3,)), dma((3,)), dma((3,)), dma((3, N, 2)), dma((3,))],
            compiler_params=params,
        )(x, rows, meta)
        out = pl.pallas_call(
            functools.partial(_experts, cols),
            name='experts',
            out_shape=[jax.ShapeDtypeStruct((T, D), BF16)] + [jax.ShapeDtypeStruct((N, K * C, w), BF16) for w in widths]
            + [jax.ShapeDtypeStruct((N, len(LATER), C, w), BF16) for w in widths],
            in_specs=[any_] * 4 + [vmem],
            out_specs=[vmem] + [any_] * 6,
            scratch_shapes=[
                pltpu.VMEM((D, ff), BF16), pltpu.VMEM((D, ff), BF16), pltpu.VMEM((ff, D), BF16),
                pltpu.VMEM((2, 2, N, 2, C, D), BF16), pltpu.VMEM((2 * L, ff), BF16), pltpu.VMEM((N, N, N, 2, C, D), BF16),
                *(pltpu.VMEM((N, len(ONCE), C, w), BF16) for w in widths),
                *(pltpu.VMEM((N, T, w), F32) for w in widths), *(pltpu.VMEM((2, T, w), F32) for w in widths),
                *(pltpu.VMEM((2, T // 2, w), F32) for w in widths),
                dma((3,)), dma((2, 2)), dma((3,)), dma((3,)), dma((3,)), dma((3,)), dma((3,)), dma((3, len(ONCE))), dma((3, len(LATER))), dma((3,)),
                dma((N,)), dma((3, 6)), dma((3, 6)),
            ],
            compiler_params=params,
        )(xin, w1, w3, w2, metas)
        return out[0]

    return jax.shard_map(local, mesh=mesh, in_specs=(tok, P(None, None), tok, wsp, wsp, wsp), out_specs=tok, check_vma=False)
```
